256 devices in a mesh: space: 32 (over z, y_hi, core), tm: 8 (over x, y_lo).
Axes of the slice: x: 4, y: 4 (y_hi: 2, y_lo: 2; y = y_hi * 2 + y_lo), z: 8, core: 2. Of those that a mesh axis runs over, the one named last changes fastest.
Arguments:
- solutions: bfloat16 [8, 12, 16384, 128], P('tm', None, 'space'), may hold values from -6 to 6
- noise: int32 [8, 64, 12, 16384], P('tm', None, None, 'space'), may hold values from 0 to 3
- momenta: int32 [27, 3], replicated, may hold values from -2 to 2
- pairs: int32 [64, 2], P('tm'), may hold values from 0 to 7
Outputs:
- mesons: float32 [8, 2, 27, 64, 64], P('tm', None, None, 'space')
- correlators: float32 [64, 2, 27], P('tm')
The draws below stay inside these ranges and needn't reach their ends.
All inputs are finite; a program needn't handle non-finite values.
Results may differ from the reference program's by a relative error of at most 0.002.
Values sent between devices are 32-bit elements; how exact they have to be, the bound alone decides.
A program may use at most 64 MiB of HBM per device.

```python
import math
import jax
import jax.numpy as jnp
from jax import lax

NVEC = 64
SPINCOL = 12
MOMS = 27
EXTENT = 48
SITES = 16384
TSL = 8
NPAIRS = 64


def plant(drawn, rng, least, top_value):
    place = [jax.random.randint(jax.random.fold_in(rng, axis), (), 0, length) for axis, length in enumerate(drawn.shape)]
    main_axis = drawn.shape.index(max(drawn.shape))
    next_to = place[:main_axis] + [(place[main_axis] + 1) % drawn.shape[main_axis]] + place[main_axis + 1:]
    return drawn.at[tuple(place)].set(least).at[tuple(next_to)].set(top_value)


def level_of(key, extent, cuts, least, top_value):
    gain, own = 1.0, jax.random.fold_in(key, 6)
    for dim, parts in cuts:
        draws = jnp.exp(jax.random.uniform(jax.random.fold_in(own, dim), (parts,), jnp.float32, least / len(cuts), top_value / len(cuts)))
        gain = gain * jnp.repeat(draws, extent[dim] // parts).reshape([-1 if axis == dim else 1 for axis in range(len(extent))])
    return gain


def bell_draw(key, dims, scale, reach, split=(), held_as=jnp.bfloat16):
    result = jax.random.normal(key, dims, jnp.float32) * scale
    if len(split) > 0:
        result = level_of(key, dims, split, -0.22, 0.18) * result
    return jnp.clip(result, min=-reach, max=reach).astype(held_as)


def setup_inputs(seed: int = 0) -> dict:
    splits = jax.random.split(jax.random.key(seed), 5)
    return {
        "solutions": bell_draw(splits[0], (TSL, SPINCOL, SITES, 2 * NVEC), 1.0, 6.0, ((0, 8), (2, 32))),
        "noise": plant(jax.random.randint(splits[1], (TSL, NVEC, SPINCOL, SITES), 0, 4), jax.random.fold_in(splits[1], 1), 0, 3).astype(jnp.int32),
        "momenta": plant(jax.random.randint(splits[2], (MOMS, 3), -2, 3), jax.random.fold_in(splits[2], 1), -2, 2).astype(jnp.int32),
        "pairs": plant(jax.random.randint(splits[3], (NPAIRS, 2), 0, TSL), jax.random.fold_in(splits[3], 1), 0, TSL - 1).astype(jnp.int32),
    }


def phase_weights(noise_block, momenta, coords):
    qdotx = momenta[:, 0:1] * coords[0][None, :] + momenta[:, 1:2] * coords[1][None, :] + momenta[:, 2:3] * coords[2][None, :]
    index = (EXTENT // 4 * noise_block[None, :, :, :] + qdotx[:, None, None, :]) % EXTENT
    angle = index.astype(jnp.float32) * jnp.float32(2.0 * math.pi / EXTENT)
    rows = momenta.shape[0] * noise_block.shape[0]
    cols = noise_block.shape[1] * noise_block.shape[2]
    weight_re = jnp.cos(angle).astype(jnp.bfloat16).reshape(rows, cols)
    weight_im = (-jnp.sin(angle)).astype(jnp.bfloat16).reshape(rows, cols)
    return (weight_re, weight_im)

def site_coords(first, count):
    glob = first + jnp.arange(count, dtype=jnp.int32)
    return (glob % EXTENT, glob // EXTENT % EXTENT, glob // (EXTENT * EXTENT))

def slice_field(vectors, sources, momenta):
    block = min(1024, SITES)
    nblocks = SITES // block

    def one_block(step, total):
        first = (step * block).astype(jnp.int32)
        noise_block = lax.dynamic_slice_in_dim(sources, first, block, 2)
        vec_block = lax.dynamic_slice_in_dim(vectors, first, block, 1)
        weight_re, weight_im = phase_weights(noise_block, momenta, site_coords(first, block))
        stacked = vec_block.reshape(SPINCOL * block, 2 * NVEC)
        left = jnp.dot(weight_re, stacked, preferred_element_type=jnp.float32)
        right = jnp.dot(weight_im, stacked, preferred_element_type=jnp.float32)
        real_part = left[:, :NVEC] - right[:, NVEC:]
        imag_part = left[:, NVEC:] + right[:, :NVEC]
        return total + jnp.stack([real_part, imag_part], 0)
    start = jnp.zeros((2, MOMS * NVEC, NVEC), jnp.float32)
    total = lax.fori_loop(0, nblocks, one_block, start)
    return total.reshape(2, MOMS, NVEC, NVEC)

def reference(solutions, noise, momenta, pairs):
    scale = 1.0 / math.sqrt(SPINCOL * SITES)
    fields = [slice_field(solutions[t], noise[t], momenta) * scale for t in range(TSL)]
    mesons = jnp.stack(fields, 0)
    sink = mesons[pairs[:, 1]]
    source = mesons[pairs[:, 0]]
    real_part = lax.optimization_barrier(jnp.sum(sink[:, 0] * source[:, 0] + sink[:, 1] * source[:, 1], axis=(2, 3)))
    imag_part = lax.optimization_barrier(jnp.sum(sink[:, 1] * source[:, 0] - sink[:, 0] * source[:, 1], axis=(2, 3)))
    correlators = jnp.stack([real_part, imag_part], 1) / NVEC
    return (mesons, correlators)
```

```python
import functools, math
import numpy as np
import jax, jax.numpy as jnp
from jax import lax
from jax.experimental import pallas as pl
from jax.experimental.pallas import tpu as pltpu
from jax.sharding import PartitionSpec as P

EXTENT = 48
S1, S2 = 1.625, 1.1325


def twiddles():
    table = np.zeros((3, 8, 128), np.float32)
    for ph in range(3):
        x = 16 * ph + np.arange(64)
        x = np.concatenate([x, x])
        a = 2 * np.pi * x / EXTENT
        table[ph, 0] = S1 * np.cos(a)
        table[ph, 1] = S1 * np.sin(a)
        table[ph, 2] = S2 * np.cos(2 * a)
        table[ph, 3] = S2 * np.sin(2 * a)
    return table


def turned(v):
    return jnp.concatenate([-v[:, 64:], v[:, :64]], axis=1)


def field_kernel(mom_ref, kap_ref, noise_ref, v_ref, tw_ref, out_ref, lhs, rhs, hrow):
    phase0 = lax.rem(lax.axis_index("space") * 32, 48)
    hrow[...] = jnp.zeros_like(hrow)

    def tile(lt, _):
        lane0 = pl.multiple_of(lt * 128, 128)
        for aq in range(3):
            n = [noise_ref[4 * aq + a, :, pl.ds(lane0, 128)].astype(jnp.float32).astype(jnp.bfloat16) for a in range(4)]
            for h in range(2):
                start = phase0 + lt * 128 + h * 64
                ph = lax.rem(start, 48) // 16
                tw = tw_ref[ph].astype(jnp.bfloat16)
                cut = slice(64 * h, 64 * h + 64)
                for pair in range(2):
                    both = jnp.concatenate([n[2 * pair][:, cut], n[2 * pair + 1][:, cut]], axis=1)
                    zr = jnp.abs(both - 2) - 1
                    zi = jnp.abs(both - 1) - 1
                    at = aq * 512 + pair * 128
                    for f in range(5):
                        rows = pl.ds(64 * f, 64)
                        if f == 0:
                            left, right = zr, zi
                        else:
                            w = tw[f - 1 : f, :]
                            if f % 2 == 1:
                                left, right = zr * w, zi * w
                            else:
                                left, right = zi * (-w), zr * w
                        lhs[h, rows, at : at + 128] = left
                        lhs[h, rows, at + 256 : at + 384] = right
                for a in range(4):
                    for g in range(4):
                        v = v_ref[4 * aq + a, pl.ds(pl.multiple_of(lt * 128 + h * 64 + 16 * g, 16), 16), :]
                        t = turned(v)
                        first = 16 * g < 48 - 16 * ph
                        zero = jnp.zeros_like(v)
                        at = aq * 512 + 64 * a + 16 * g
                        rhs[h, at : at + 16, 0:128] = jnp.where(first, v, zero)
                        rhs[h, at : at + 16, 128:256] = jnp.where(first, zero, v)
                        rhs[h, at + 256 : at + 272, 0:128] = jnp.where(first, t, zero)
                        rhs[h, at + 256 : at + 272, 128:256] = jnp.where(first, zero, t)
        for h in range(2):
            start = phase0 + lt * 128 + h * 64
            row = start // 48
            out = jnp.dot(lhs[h], rhs[h], preferred_element_type=jnp.float32)
            g = [out[64 * f : 64 * f + 64, :] for f in range(5)]
            terms = [g[3] + g[4], g[1] + g[2], g[0], g[1] - g[2], g[3] - g[4]]
            for q0 in range(5):
                for r in range(2):
                    hrow[q0, row + r] += terms[q0][:, 128 * r : 128 * r + 128]
        return 0

    lax.fori_loop(0, 4, tile, 0)

    def momentum(q, _):
        q0 = mom_ref[3 * q] + 2
        acc_r = jnp.zeros((64, 128), jnp.float32)
        acc_i = jnp.zeros((64, 128), jnp.float32)
        for row in range(12):
            part = hrow[q0, row]
            acc_r += kap_ref[24 * q + 2 * row] * part
            acc_i += kap_ref[24 * q + 2 * row + 1] * part
        out_ref[q] = acc_r + turned(acc_i)
        return 0

    lax.fori_loop(0, 27, momentum, 0)


def row_phases(momenta, scale):
    first = lax.axis_index("space") * 512 // EXTENT
    row = first + jnp.arange(12, dtype=jnp.int32)
    y, z = row % EXTENT, row // EXTENT
    m = (momenta[:, 1:2] * y + momenta[:, 2:3] * z) % EXTENT
    angle = m.astype(jnp.float32) * jnp.float32(2.0 * math.pi / EXTENT)
    q0 = jnp.abs(momenta[:, 0:1])
    size = jnp.where(q0 == 0, scale, jnp.where(q0 == 1, scale / S1, scale / S2)).astype(jnp.float32)
    return jnp.stack([jnp.cos(angle) * size, -jnp.sin(angle) * size], axis=2)


def partial_field(solutions, noise, momenta, scale):
    kap = row_phases(momenta, scale).reshape(-1)
    vmem = pl.BlockSpec(memory_space=pltpu.VMEM)
    smem = pl.BlockSpec(memory_space=pltpu.SMEM)
    return pl.pallas_call(
        field_kernel,
        out_shape=jax.ShapeDtypeStruct((27, 64, 128), jnp.float32),
        in_specs=[smem, smem, vmem, vmem, vmem],
        out_specs=vmem,
        scratch_shapes=[
            pltpu.VMEM((2, 320, 1536), jnp.bfloat16),
            pltpu.VMEM((2, 1536, 256), jnp.bfloat16),
            pltpu.VMEM((5, 12, 64, 128), jnp.float32),
        ],
        compiler_params=pltpu.CompilerParams(vmem_limit_bytes=40 * 1024 * 1024),
        name="fields",
    )(momenta.reshape(-1), kap, noise.transpose(1, 0, 2), solutions, jnp.asarray(twiddles()))


def in_blocks(array, dim, length):
    before, after = (array.shape[:dim], array.shape[dim + 1 :])
    return jnp.moveaxis(array.reshape(*before, length, -1, *after), dim, 0)


def summed_on_arrival(array, axis, dim):
    pieces = in_blocks(array, dim, lax.axis_size(axis))
    arrived = lax.all_to_all(pieces, axis, split_axis=0, concat_axis=0, tiled=True)
    return arrived.sum(axis=0)


def copy_for_each(array, axis):
    copies = jnp.broadcast_to(array, (lax.axis_size(axis), *array.shape))
    return lax.all_to_all(copies, axis, split_axis=0, concat_axis=0, tiled=True)


def laid_out(pieces, dim):
    pieces = jnp.moveaxis(pieces, 0, dim)
    dims = pieces.shape
    return pieces.reshape(*dims[:dim], dims[dim] * dims[dim + 1], *dims[dim + 2 :])


def gathered_copies(array, axis, dim):
    pieces = copy_for_each(array, axis)
    return laid_out(pieces, dim)


def over_copies(array, axis):
    return copy_for_each(array, axis).sum(axis=0)


def pair_traces(fields, pairs):
    nslices = fields.shape[0]
    slots = jnp.arange(nslices, dtype=jnp.int32)
    pick_sink = (pairs[:, 1][:, None] == slots[None, :]).astype(jnp.float32)
    pick_source = (pairs[:, 0][:, None] == slots[None, :]).astype(jnp.float32)
    sink = jnp.einsum("kt,tcpij->kcpij", pick_sink, fields, precision=lax.Precision.HIGHEST)
    source = jnp.einsum("kt,tcpij->kcpij", pick_source, fields, precision=lax.Precision.HIGHEST)
    real_part = jnp.sum(sink[:, 0] * source[:, 0] + sink[:, 1] * source[:, 1], axis=(2, 3))
    imag_part = jnp.sum(sink[:, 1] * source[:, 0] - sink[:, 0] * source[:, 1], axis=(2, 3))
    return jnp.stack([real_part, imag_part], 1)


def local(solutions, noise, momenta, pairs):
    nvec = noise.shape[1]
    scale = 1.0 / math.sqrt(noise.shape[2] * solutions.shape[2] * lax.axis_size("space"))
    field = partial_field(solutions[0], noise[0], momenta, scale)
    pieces = field.reshape(27, 32, 2, 128).transpose(1, 0, 2, 3).reshape(32, 54, 128)
    arrived = lax.all_to_all(pieces, "space", split_axis=0, concat_axis=0, tiled=True).sum(axis=0)
    mesons = arrived.reshape(27, 2, 2, 64).transpose(2, 0, 1, 3)[None]
    every_slice = gathered_copies(mesons, "tm", 0)
    partial_traces = pair_traces(every_slice, pairs)
    correlators = over_copies(partial_traces, "space") / nvec
    return (mesons, correlators)


def solution(mesh):
    in_specs = (P("tm", None, "space", None), P("tm", None, None, "space"), P(), P("tm", None))
    out_specs = (P("tm", None, None, "space", None), P("tm", None, None))
    return jax.shard_map(local, mesh=mesh, in_specs=in_specs, out_specs=out_specs, check_vma=False)
```

```python
import math

import jax
import jax.numpy as jnp
from jax import lax
from jax.experimental import pallas as pl
from jax.experimental.pallas import tpu as pltpu
from jax.sharding import PartitionSpec as P

EXTENT = 48
MOMS = 27
CHUNKS = 7
SIZE1, SIZE2 = 1.625, 1.1325
MESH = pl.DeviceIdType.MESH


def iota(shape, dim):
    return lax.broadcasted_iota(jnp.int32, shape, dim)


def swap_halves(array):
    return jnp.concatenate([array[:, 64:], array[:, :64]], axis=1)


def swapped(low, high, bit):
    has_bit = (iota((8, 128), 0) & bit) != 0
    return (
        jnp.where(has_bit, pltpu.roll(high, bit, 0), low),
        jnp.where(has_bit, high, pltpu.roll(low, 8 - bit, 0)),
    )


def fields_kernel(
    mom_s, pair_s, mom_v, noise_h, vec_h, mesons, traces,
    noise_v, vec_v, lhs, rhs, hrow, kap_r, kap_i,
    raw, core_in, half, y_in, own, z_in, slices, here, turned, four, eight,
    noise_sem, vec_sem, core_s, core_r, y_s, y_r, z_s, z_r, t_s, t_r, four_s, four_r, eight_s, eight_r,
):
    space, tm = lax.axis_index("space"), lax.axis_index("tm")
    z, y, core = space // 4, lax.rem(space // 2, 2), lax.rem(space, 2)
    quad = lax.rem(space, 4)

    def in_z(d):
        return {"space": lax.rem(z + d, 8) * 4 + quad, "tm": tm}

    def in_quad(d):
        return {"space": z * 4 + (quad ^ d), "tm": tm}

    def in_tm(d):
        return {"space": space, "tm": lax.rem(tm + d, 8)}

    def load(tile):
        lanes = pl.ds(tile * 128, 128)
        return (
            pltpu.make_async_copy(noise_h.at[:, :, lanes], noise_v.at[tile], noise_sem.at[tile]),
            pltpu.make_async_copy(vec_h.at[:, lanes, :], vec_v.at[tile], vec_sem.at[tile]),
        )

    for tile in range(4):
        for copy in load(tile):
            copy.start()

    barrier = pltpu.get_barrier_semaphore()
    for d in range(1, 4):
        pl.semaphore_signal(barrier, inc=1, device_id=in_quad(d), device_id_type=MESH)
    for d in range(1, 8):
        pl.semaphore_signal(barrier, inc=1, device_id=in_z(d), device_id_type=MESH)
        pl.semaphore_signal(barrier, inc=1, device_id=in_tm(d), device_id_type=MESH)

    scale = 1.0 / math.sqrt(12 * 512 * 32)
    row = space * 512 // EXTENT + iota((MOMS, 128), 1)
    q0 = jnp.abs(mom_v[:, 0:1])
    angle = (mom_v[:, 1:2] * lax.rem(row, EXTENT) + mom_v[:, 2:3] * (row // EXTENT)).astype(jnp.float32)
    angle = angle * jnp.float32(2.0 * math.pi / EXTENT)
    size = jnp.where(q0 == 0, scale, jnp.where(q0 == 1, scale / SIZE1, scale / SIZE2))
    phase_r, phase_i = jnp.cos(angle) * size, -jnp.sin(angle) * size
    left = iota((MOMS, 128), 1) < 64
    for r in range(12):
        kap_r[r] = jnp.broadcast_to(phase_r[:, r : r + 1], (MOMS, 128))
        column = jnp.broadcast_to(phase_i[:, r : r + 1], (MOMS, 128))
        kap_i[r] = jnp.where(left, column, -column)

    hrow[...] = jnp.zeros_like(hrow)
    phase0 = lax.rem(space * 32, EXTENT)
    lane = lax.rem(iota((8, 128), 1), 64)
    kind = iota((8, 128), 0)
    harmonic = jnp.where(kind < 2, 1, 2)
    amplitude = jnp.where(kind < 2, SIZE1, SIZE2)
    negate = iota((16, 128), 1) < 64

    def tile_step(tile, _):
        for copy in load(tile):
            copy.wait()
        starts = [phase0 + tile * 128 + 64 * h for h in range(2)]
        firsts = [lax.rem(start, EXTENT) for start in starts]
        waves = []
        for first in firsts:
            turn = ((first + lane) * harmonic).astype(jnp.float32) * jnp.float32(2.0 * math.pi / EXTENT)
            waves.append((amplitude * jnp.where(kind % 2 == 0, jnp.cos(turn), jnp.sin(turn))).astype(jnp.bfloat16))
        for a4 in range(3):
            n = [noise_v[tile, 4 * a4 + a].astype(jnp.float32).astype(jnp.bfloat16) for a in range(4)]
            for h in range(2):
                cut = slice(64 * h, 64 * h + 64)
                for two in range(2):
                    both = jnp.concatenate([n[2 * two][:, cut], n[2 * two + 1][:, cut]], axis=1)
                    z4_r, z4_i = jnp.abs(both - 2) - 1, jnp.abs(both - 1) - 1
                    at = a4 * 512 + two * 128
                    for f in range(5):
                        rows = pl.ds(64 * f, 64)
                        if f == 0:
                            first_part, second_part = z4_r, z4_i
                        else:
                            wave = waves[h][f - 1 : f, :]
                            if f % 2 == 1:
                                first_part, second_part = z4_r * wave, z4_i * wave
                            else:
                                first_part, second_part = z4_i * (-wave), z4_r * wave
                        lhs[h, rows, at : at + 128] = first_part
                        lhs[h, rows, at + 256 : at + 384] = second_part
                for a in range(4):
                    for g in range(4):
                        v = vec_v[tile, 4 * a4 + a, 64 * h + 16 * g : 64 * h + 16 * g + 16, :]
                        t = swap_halves(v)
                        t = jnp.where(negate, -t, t)
                        in_first = firsts[h] + 16 * g < EXTENT
                        zero = jnp.zeros_like(v)
                        at = a4 * 512 + 64 * a + 16 * g
                        rhs[h, at : at + 16, 0:128] = jnp.where(in_first, v, zero)
                        rhs[h, at : at + 16, 128:256] = jnp.where(in_first, zero, v)
                        rhs[h, at + 256 : at + 272, 0:128] = jnp.where(in_first, t, zero)
                        rhs[h, at + 256 : at + 272, 128:256] = jnp.where(in_first, zero, t)
        for h in range(2):
            out = jnp.dot(lhs[h], rhs[h], preferred_element_type=jnp.float32)
            f = [out[64 * k : 64 * k + 64, :] for k in range(5)]
            terms = [f[3] + f[4], f[1] + f[2], f[0], f[1] - f[2], f[3] - f[4]]
            for k in range(5):
                for r in range(2):
                    hrow[k, starts[h] // EXTENT + r] += terms[k][:, 128 * r : 128 * r + 128]
        return 0

    lax.fori_loop(0, 4, tile_step, 0)
    pl.semaphore_wait(barrier, 17)

    def to_core(g):
        return pltpu.make_async_remote_copy(
            src_ref=raw.at[1 - core, g], dst_ref=core_in.at[g], send_sem=core_s.at[g], recv_sem=core_r.at[g],
            device_id=in_quad(1), device_id_type=MESH,
        )

    def to_y(g):
        return pltpu.make_async_remote_copy(
            src_ref=half.at[g, 1 - y], dst_ref=y_in.at[g], send_sem=y_s.at[g], recv_sem=y_r.at[g],
            device_id=in_quad(2), device_id_type=MESH,
        )

    def to_z(g, d):
        return pltpu.make_async_remote_copy(
            src_ref=own.at[g, lax.rem(z + d, 8)], dst_ref=z_in.at[g, d - 1],
            send_sem=z_s.at[g, d - 1], recv_sem=z_r.at[g, d - 1], device_id=in_z(d), device_id_type=MESH,
        )

    def to_tm(g, d):
        return pltpu.make_async_remote_copy(
            src_ref=slices.at[g, tm], dst_ref=slices.at[g, tm],
            send_sem=t_s.at[g, d - 1], recv_sem=t_r.at[g, d - 1], device_id=in_tm(d), device_id_type=MESH,
        )

    def momentum(g, k):
        q = lax.min(4 * g + k, MOMS - 1)
        q0 = mom_s[0, q] + 2
        acc_r = [jnp.zeros((8, 128), jnp.float32) for _ in range(8)]
        acc_i = [jnp.zeros((8, 128), jnp.float32) for _ in range(8)]
        for r in range(12):
            k_r = jnp.broadcast_to(kap_r[r, pl.ds(q, 1), :], (8, 128))
            k_i = jnp.broadcast_to(kap_i[r, pl.ds(q, 1), :], (8, 128))
            for i in range(8):
                part = hrow[q0, r, 8 * i : 8 * i + 8, :]
                acc_r[i] += k_r * part
                acc_i[i] += k_i * part
        tiles = [acc_r[i] + swap_halves(acc_i[i]) for i in range(8)]
        by_core = [swapped(tiles[2 * i], tiles[2 * i + 1], 2) for i in range(4)]
        for c in range(2):
            for i in range(2):
                by_y = swapped(by_core[2 * i][c], by_core[2 * i + 1][c], 4)
                for yy in range(2):
                    raw[c, g, yy, k, 8 * i : 8 * i + 8, :] = by_y[yy]

    def after_core(g):
        to_core(g).wait_recv()
        for yy in range(2):
            half[g, yy] = raw[core, g, yy] + core_in[g, yy]
        to_y(g).start()

    def first_step(g, _):
        def one(k, _):
            momentum(g, k)
            return 0

        lax.fori_loop(0, 4, one, 0)
        to_core(g).start()

        @pl.when(g >= 1)
        def _():
            after_core(g - 1)

        return 0

    lax.fori_loop(0, CHUNKS, first_step, 0)
    after_core(CHUNKS - 1)

    def after_y(g, _):
        to_y(g).wait_recv()
        sums = half[g, y] + y_in[g]
        for top in range(2):
            tiles = [sums[k, 8 * top : 8 * top + 8, :] for k in range(4)]
            low = [swapped(tiles[2 * k], tiles[2 * k + 1], 2) for k in range(2)]
            for bit in range(2):
                pair = swapped(low[0][bit], low[1][bit], 4)
                for upper in range(2):
                    own[g, 4 * top + 2 * upper + bit] = pair[upper]
        for d in range(1, 8):
            to_z(g, d).start()
        return 0

    lax.fori_loop(0, CHUNKS, after_y, 0)

    def after_z(g, _):
        total = own[g, z]
        for d in range(1, 8):
            to_z(g, d).wait_recv()
            total += z_in[g, d - 1]
        mesons[g] = total
        slices[g, tm] = total
        for d in range(1, 8):
            to_tm(g, d).start()
        return 0

    lax.fori_loop(0, CHUNKS, after_z, 0)

    lanes = iota((8, 128), 1)

    def after_tm(g, sums):
        for d in range(1, 8):
            to_tm(g, d).wait_recv()
        for t in range(8):
            tile = slices[g, t]
            here[t] = tile
            turned[t] = swap_halves(jnp.where(lanes < 64, tile, -tile))
        for k in range(8):
            sink, source, rotated = here[pair_s[1, k]], here[pair_s[0, k]], turned[pair_s[0, k]]
            for c, term in enumerate((sink * source, sink * rotated)):
                value = jnp.sum(term, axis=1, keepdims=True)
                sums = jnp.where(lanes == (2 * k + c) * CHUNKS + g, value, sums)
        return sums

    four[quad] = lax.fori_loop(0, CHUNKS, after_tm, jnp.zeros((8, 128), jnp.float32))

    def to_quad(d):
        return pltpu.make_async_remote_copy(
            src_ref=four.at[quad], dst_ref=four.at[quad], send_sem=four_s.at[d - 1], recv_sem=four_r.at[d - 1],
            device_id=in_quad(d), device_id_type=MESH,
        )

    def to_all_z(d):
        return pltpu.make_async_remote_copy(
            src_ref=eight.at[z], dst_ref=eight.at[z], send_sem=eight_s.at[d - 1], recv_sem=eight_r.at[d - 1],
            device_id=in_z(d), device_id_type=MESH,
        )

    for d in range(1, 4):
        to_quad(d).start()
    for d in range(1, 4):
        to_quad(d).wait_recv()
    eight[z] = (four[0] + four[1]) + (four[2] + four[3])
    for d in range(1, 8):
        to_all_z(d).start()
    for d in range(1, 8):
        to_all_z(d).wait_recv()
    total = eight[0]
    for k in range(1, 8):
        total += eight[k]
    traces[...] = total * (1.0 / 64)

    def finish(g, _):
        to_core(g).wait_send()
        to_y(g).wait_send()
        for d in range(1, 8):
            to_z(g, d).wait_send()
            to_tm(g, d).wait_send()
        return 0

    lax.fori_loop(0, CHUNKS, finish, 0)
    for d in range(1, 4):
        to_quad(d).wait_send()
    for d in range(1, 8):
        to_all_z(d).wait_send()


def local(solutions, noise, momenta, pairs):
    f32, bf16 = jnp.float32, jnp.bfloat16
    vmem = pl.BlockSpec(memory_space=pltpu.VMEM)
    smem = pl.BlockSpec(memory_space=pltpu.SMEM)
    hbm = pl.BlockSpec(memory_space=pl.ANY)
    dma = pltpu.SemaphoreType.DMA
    mesons, traces = pl.pallas_call(
        fields_kernel,
        out_shape=(
            jax.ShapeDtypeStruct((CHUNKS, 8, 128), f32),
            jax.ShapeDtypeStruct((8, 128), f32),
        ),
        in_specs=[smem, smem, vmem, hbm, hbm],
        out_specs=(vmem, vmem),
        scratch_shapes=[
            pltpu.VMEM((4, 12, 64, 128), jnp.int32),
            pltpu.VMEM((4, 12, 128, 128), bf16),
            pltpu.VMEM((2, 320, 1536), bf16),
            pltpu.VMEM((2, 1536, 256), bf16),
            pltpu.VMEM((5, 12, 64, 128), f32),
            pltpu.VMEM((12, MOMS, 128), f32),
            pltpu.VMEM((12, MOMS, 128), f32),
            pltpu.VMEM((2, CHUNKS, 2, 4, 16, 128), f32),
            pltpu.VMEM((CHUNKS, 2, 4, 16, 128), f32),
            pltpu.VMEM((CHUNKS, 2, 4, 16, 128), f32),
            pltpu.VMEM((CHUNKS, 4, 16, 128), f32),
            pltpu.VMEM((CHUNKS, 8, 8, 128), f32),
            pltpu.VMEM((CHUNKS, 7, 8, 128), f32),
            pltpu.VMEM((CHUNKS, 8, 8, 128), f32),
            pltpu.VMEM((8, 8, 128), f32),
            pltpu.VMEM((8, 8, 128), f32),
            pltpu.VMEM((4, 8, 128), f32),
            pltpu.VMEM((8, 8, 128), f32),
            dma((4,)), dma((4,)),
            dma((CHUNKS,)), dma((CHUNKS,)),
            dma((CHUNKS,)), dma((CHUNKS,)),
            dma((CHUNKS, 7)), dma((CHUNKS, 7)),
            dma((CHUNKS, 7)), dma((CHUNKS, 7)),
            dma((3,)), dma((3,)),
            dma((7,)), dma((7,)),
        ],
        compiler_params=pltpu.CompilerParams(
            collective_id=0, has_side_effects=True, vmem_limit_bytes=40 * 1024 * 1024
        ),
        name="meson_fields",
    )(momenta.T, pairs.T, momenta, noise[0].transpose(1, 0, 2), solutions[0])
    mesons = mesons.reshape(4 * CHUNKS, 2, 2, 64)[:MOMS].transpose(2, 0, 1, 3)[None]
    traces = traces.reshape(4, 2, 128).sum(axis=1)[:, : 16 * CHUNKS].reshape(4, 16, CHUNKS)
    correlators = traces.transpose(1, 2, 0).reshape(8, 2, 4 * CHUNKS)[:, :, :MOMS]
    return (mesons, correlators)


def solution(mesh):
    in_specs = (P("tm", None, "space", None), P("tm", None, None, "space"), P(), P("tm", None))
    out_specs = (P("tm", None, None, "space", None), P("tm", None, None))
    return jax.shard_map(local, mesh=mesh, in_specs=in_specs, out_specs=out_specs, check_vma=False)
```

```python
import math

import jax
import jax.numpy as jnp
from jax import lax
from jax.experimental import pallas as pl
from jax.experimental.pallas import tpu as pltpu
from jax.sharding import PartitionSpec as P

EXTENT = 48
MOMS = 27
CHUNKS = 7
SIZE1, SIZE2 = 1.625, 1.1325
MESH = pl.DeviceIdType.MESH
PLANE = [(e, d) for e in range(2) for d in range(8) if (e, d) != (0, 0)]


def iota(shape, dim):
    return lax.broadcasted_iota(jnp.int32, shape, dim)


def swap_halves(array):
    return jnp.concatenate([array[:, 64:], array[:, :64]], axis=1)


def swapped(low, high, bit):
    has_bit = (iota((8, 128), 0) & bit) != 0
    return (
        jnp.where(has_bit, pltpu.roll(high, bit, 0), low),
        jnp.where(has_bit, high, pltpu.roll(low, 8 - bit, 0)),
    )


def fields_kernel(
    mom_h, pair_h, noise_h, vec_h, mesons, traces,
    mom_s, pair_s, spread, noise_v, vec_v, lhs, rhs, hrow, kap_r, kap_i,
    sums, raw, core_in, own, z_in, mine, slices, here, turned, both, chips,
    small_sem, noise_sem, vec_sem, core_s, core_r, z_s, z_r, t_s, t_r, last_s, last_r,
):
    space, tm = lax.axis_index("space"), lax.axis_index("tm")
    z, y, core = space // 4, lax.rem(space // 2, 2), lax.rem(space, 2)
    quad = lax.rem(space, 4)

    def in_z(d):
        return {"space": lax.rem(z + d, 8) * 4 + quad, "tm": tm}

    def in_quad(d):
        return {"space": z * 4 + (quad ^ d), "tm": tm}

    def in_plane(e, d):
        return {"space": space ^ (2 * e), "tm": lax.rem(tm + d, 8)}

    def in_chips(e, d):
        return {"space": (lax.rem(z + d, 8) * 4 + quad) ^ (2 * e), "tm": tm}

    def load(tile):
        lanes = pl.ds(tile * 128, 128)
        return (
            pltpu.make_async_copy(noise_h.at[:, :, lanes], noise_v.at[tile], noise_sem.at[tile]),
            pltpu.make_async_copy(vec_h.at[:, lanes, :], vec_v.at[tile], vec_sem.at[tile]),
        )

    small = (
        pltpu.make_async_copy(mom_h, mom_s, small_sem.at[0]),
        pltpu.make_async_copy(pair_h, pair_s, small_sem.at[1]),
    )
    for copy in small:
        copy.start()
    for tile in range(4):
        for copy in load(tile):
            copy.start()

    barrier = pltpu.get_barrier_semaphore()
    pl.semaphore_signal(barrier, inc=1, device_id=in_quad(1), device_id_type=MESH)
    for e, d in PLANE:
        pl.semaphore_signal(barrier, inc=1, device_id=in_chips(e, d), device_id_type=MESH)
        if d > 0:
            pl.semaphore_signal(barrier, inc=1, device_id=in_plane(e, d), device_id_type=MESH)

    hrow[...] = jnp.zeros_like(hrow)
    for copy in small:
        copy.wait()
    for q in range(MOMS):
        for k in range(3):
            spread[k, q : q + 1, :] = jnp.full((1, 128), mom_s[k, q], jnp.int32)

    scale = 1.0 / math.sqrt(12 * 512 * 32)
    row = space * 512 // EXTENT + iota((MOMS, 128), 1)
    q0 = jnp.abs(spread[0])
    angle = (spread[1] * lax.rem(row, EXTENT) + spread[2] * (row // EXTENT)).astype(jnp.float32)
    angle = angle * jnp.float32(2.0 * math.pi / EXTENT)
    size = jnp.where(q0 == 0, scale, jnp.where(q0 == 1, scale / SIZE1, scale / SIZE2))
    phase_r, phase_i = jnp.cos(angle) * size, -jnp.sin(angle) * size
    left = iota((MOMS, 128), 1) < 64
    for r in range(12):
        kap_r[r] = jnp.broadcast_to(phase_r[:, r : r + 1], (MOMS, 128))
        column = jnp.broadcast_to(phase_i[:, r : r + 1], (MOMS, 128))
        kap_i[r] = jnp.where(left, column, -column)

    phase0 = lax.rem(space * 32, EXTENT)
    lane = lax.rem(iota((8, 128), 1), 64)
    kind = iota((8, 128), 0)
    harmonic = jnp.where(kind < 2, 1, 2)
    amplitude = jnp.where(kind < 2, SIZE1, SIZE2)
    negate = iota((16, 128), 1) < 64

    def tile_step(tile, _):
        for copy in load(tile):
            copy.wait()
        starts = [phase0 + tile * 128 + 64 * h for h in range(2)]
        firsts = [lax.rem(start, EXTENT) for start in starts]
        waves = []
        for first in firsts:
            turn = ((first + lane) * harmonic).astype(jnp.float32) * jnp.float32(2.0 * math.pi / EXTENT)
            waves.append((amplitude * jnp.where(kind % 2 == 0, jnp.cos(turn), jnp.sin(turn))).astype(jnp.bfloat16))
        for a4 in range(3):
            n = [noise_v[tile, 4 * a4 + a].astype(jnp.float32).astype(jnp.bfloat16) for a in range(4)]
            for h in range(2):
                cut = slice(64 * h, 64 * h + 64)
                for two in range(2):
                    both = jnp.concatenate([n[2 * two][:, cut], n[2 * two + 1][:, cut]], axis=1)
                    z4_r, z4_i = jnp.abs(both - 2) - 1, jnp.abs(both - 1) - 1
                    at = a4 * 512 + two * 128
                    for f in range(5):
                        rows = pl.ds(64 * f, 64)
                        if f == 0:
                            first_part, second_part = z4_r, z4_i
                        else:
                            wave = waves[h][f - 1 : f, :]
                            if f % 2 == 1:
                                first_part, second_part = z4_r * wave, z4_i * wave
                            else:
                                first_part, second_part = z4_i * (-wave), z4_r * wave
                        lhs[h, rows, at : at + 128] = first_part
                        lhs[h, rows, at + 256 : at + 384] = second_part
                for a in range(4):
                    for g in range(4):
                        v = vec_v[tile, 4 * a4 + a, 64 * h + 16 * g : 64 * h + 16 * g + 16, :]
                        t = swap_halves(v)
                        t = jnp.where(negate, -t, t)
                        in_first = firsts[h] + 16 * g < EXTENT
                        zero = jnp.zeros_like(v)
                        at = a4 * 512 + 64 * a + 16 * g
                        rhs[h, at : at + 16, 0:128] = jnp.where(in_first, v, zero)
                        rhs[h, at : at + 16, 128:256] = jnp.where(in_first, zero, v)
                        rhs[h, at + 256 : at + 272, 0:128] = jnp.where(in_first, t, zero)
                        rhs[h, at + 256 : at + 272, 128:256] = jnp.where(in_first, zero, t)
        for h in range(2):
            out = jnp.dot(lhs[h], rhs[h], preferred_element_type=jnp.float32)
            f = [out[64 * k : 64 * k + 64, :] for k in range(5)]
            terms = [f[3] + f[4], f[1] + f[2], f[0], f[1] - f[2], f[3] - f[4]]
            for k in range(5):
                for r in range(2):
                    hrow[k, starts[h] // EXTENT + r] += terms[k][:, 128 * r : 128 * r + 128]
        return 0

    lax.fori_loop(0, 4, tile_step, 0)
    pl.semaphore_wait(barrier, 30)

    def to_core(g):
        return pltpu.make_async_remote_copy(
            src_ref=raw.at[1 - core, g], dst_ref=core_in.at[g], send_sem=core_s.at[g], recv_sem=core_r.at[g],
            device_id=in_quad(1), device_id_type=MESH,
        )

    def to_z(g, d):
        return pltpu.make_async_remote_copy(
            src_ref=own.at[g, lax.rem(z + d, 8)], dst_ref=z_in.at[g, d - 1],
            send_sem=z_s.at[g, d - 1], recv_sem=z_r.at[g, d - 1], device_id=in_z(d), device_id_type=MESH,
        )

    def to_plane(g, e, d):
        return pltpu.make_async_remote_copy(
            src_ref=mine.at[g, y ^ e], dst_ref=slices.at[g, y, tm],
            send_sem=t_s.at[g, e, d], recv_sem=t_r.at[g, e, d], device_id=in_plane(e, d), device_id_type=MESH,
        )

    def momentum(g, k):
        q = lax.min(4 * g + k, MOMS - 1)
        q0 = mom_s[0, q] + 2
        acc_r = [jnp.zeros((8, 128), jnp.float32) for _ in range(8)]
        acc_i = [jnp.zeros((8, 128), jnp.float32) for _ in range(8)]
        for r in range(12):
            k_r = jnp.broadcast_to(kap_r[r, pl.ds(q, 1), :], (8, 128))
            k_i = jnp.broadcast_to(kap_i[r, pl.ds(q, 1), :], (8, 128))
            for i in range(8):
                part = hrow[q0, r, 8 * i : 8 * i + 8, :]
                acc_r[i] += k_r * part
                acc_i[i] += k_i * part
        for i in range(8):
            sums[k, i] = acc_r[i] + swap_halves(acc_i[i])

    def after_core(g):
        to_core(g).wait_recv()
        own[g] = raw[core, g] + core_in[g]
        for d in range(1, 8):
            to_z(g, d).start()

    def first_step(g, _):
        def one(k, _):
            momentum(g, k)
            return 0

        lax.fori_loop(0, 4, one, 0)
        for i in range(8):
            low = [swapped(sums[2 * k, i], sums[2 * k + 1, i], 2) for k in range(2)]
            for c in range(2):
                pair = swapped(low[0][c], low[1][c], 4)
                for yy in range(2):
                    raw[c, g, i, yy] = pair[yy]
        to_core(g).start()

        @pl.when(g >= 1)
        def _():
            after_core(g - 1)

        return 0

    lax.fori_loop(0, CHUNKS, first_step, 0)
    after_core(CHUNKS - 1)

    def after_z(g, _):
        total = own[g, z]
        for d in range(1, 8):
            to_z(g, d).wait_recv()
            total += z_in[g, d - 1]
        mine[g] = total
        slices[g, y, tm] = mine[g, y]
        for e, d in PLANE:
            to_plane(g, e, d).start()
        return 0

    lax.fori_loop(0, CHUNKS, after_z, 0)

    lanes = iota((8, 128), 1)

    def after_plane(g, result):
        for e, d in PLANE:
            to_plane(g, e, d).wait_recv()
        for t in range(8):
            tile = slices[g, 0, t] + slices[g, 1, t]
            here[t] = tile
            turned[t] = swap_halves(jnp.where(lanes < 64, tile, -tile))
        mesons[g] = slices[g, 0, tm] + slices[g, 1, tm]
        for k in range(8):
            sink, source, rotated = here[pair_s[1, k]], here[pair_s[0, k]], turned[pair_s[0, k]]
            for c, term in enumerate((sink * source, sink * rotated)):
                value = jnp.sum(term, axis=1, keepdims=True)
                result = jnp.where(lanes == (2 * k + c) * CHUNKS + g, value, result)
        return result

    result = lax.fori_loop(0, CHUNKS, after_plane, jnp.zeros((8, 128), jnp.float32))
    result = result + pltpu.roll(result, 7, 0)
    for k in range(4):
        both[core, k : k + 1, :] = result[2 * k : 2 * k + 1, :]

    to_other = pltpu.make_async_remote_copy(
        src_ref=both.at[core], dst_ref=both.at[core], send_sem=last_s.at[0], recv_sem=last_r.at[0],
        device_id=in_quad(1), device_id_type=MESH,
    )
    chip = z * 2 + y

    def to_chip(e, d):
        return pltpu.make_async_remote_copy(
            src_ref=chips.at[chip], dst_ref=chips.at[chip], send_sem=last_s.at[8 * e + d], recv_sem=last_r.at[8 * e + d],
            device_id=in_chips(e, d), device_id_type=MESH,
        )

    to_other.start()
    to_other.wait_recv()
    chips[chip] = both[0] + both[1]
    for e, d in PLANE:
        to_chip(e, d).start()
    for e, d in PLANE:
        to_chip(e, d).wait_recv()
    total = chips[0]
    for k in range(1, 16):
        total += chips[k]
    traces[...] = total * (1.0 / 64)

    def finish(g, _):
        to_core(g).wait_send()
        for d in range(1, 8):
            to_z(g, d).wait_send()
        for e, d in PLANE:
            to_plane(g, e, d).wait_send()
        return 0

    lax.fori_loop(0, CHUNKS, finish, 0)
    to_other.wait_send()
    for e, d in PLANE:
        to_chip(e, d).wait_send()


def local(solutions, noise, momenta, pairs):
    f32, bf16 = jnp.float32, jnp.bfloat16
    vmem = pl.BlockSpec(memory_space=pltpu.VMEM)
    hbm = pl.BlockSpec(memory_space=pltpu.HBM)
    dma = pltpu.SemaphoreType.DMA
    mesons, traces = pl.pallas_call(
        fields_kernel,
        out_shape=(
            jax.ShapeDtypeStruct((CHUNKS, 8, 128), f32),
            jax.ShapeDtypeStruct((4, 128), f32),
        ),
        in_specs=[hbm] * 4,
        out_specs=(vmem, vmem),
        scratch_shapes=[
            pltpu.SMEM((3, MOMS), jnp.int32),
            pltpu.SMEM((2, 8), jnp.int32),
            pltpu.VMEM((3, MOMS, 128), jnp.int32),
            pltpu.VMEM((4, 12, 64, 128), jnp.int32),
            pltpu.VMEM((4, 12, 128, 128), bf16),
            pltpu.VMEM((2, 320, 1536), bf16),
            pltpu.VMEM((2, 1536, 256), bf16),
            pltpu.VMEM((5, 12, 64, 128), f32),
            pltpu.VMEM((12, MOMS, 128), f32),
            pltpu.VMEM((12, MOMS, 128), f32),
            pltpu.VMEM((4, 8, 8, 128), f32),
            pltpu.VMEM((2, CHUNKS, 8, 2, 8, 128), f32),
            pltpu.VMEM((CHUNKS, 8, 2, 8, 128), f32),
            pltpu.VMEM((CHUNKS, 8, 2, 8, 128), f32),
            pltpu.VMEM((CHUNKS, 7, 2, 8, 128), f32),
            pltpu.VMEM((CHUNKS, 2, 8, 128), f32),
            pltpu.VMEM((CHUNKS, 2, 8, 8, 128), f32),
            pltpu.VMEM((8, 8, 128), f32),
            pltpu.VMEM((8, 8, 128), f32),
            pltpu.VMEM((2, 4, 128), f32),
            pltpu.VMEM((16, 4, 128), f32),
            dma((2,)), dma((4,)), dma((4,)),
            dma((CHUNKS,)), dma((CHUNKS,)),
            dma((CHUNKS, 7)), dma((CHUNKS, 7)),
            dma((CHUNKS, 2, 8)), dma((CHUNKS, 2, 8)),
            dma((16,)), dma((16,)),
        ],
        compiler_params=pltpu.CompilerParams(
            collective_id=0, has_side_effects=True, vmem_limit_bytes=67043328
        ),
        name="meson_fields",
    )(momenta.T, pairs.T, noise[0].transpose(1, 0, 2), solutions[0])
    mesons = mesons.reshape(4 * CHUNKS, 2, 2, 64)[:MOMS].transpose(2, 0, 1, 3)[None]
    traces = traces[:, : 16 * CHUNKS].reshape(4, 16, CHUNKS)
    correlators = traces.transpose(1, 2, 0).reshape(8, 2, 4 * CHUNKS)[:, :, :MOMS]
    return (mesons, correlators)


def solution(mesh):
    in_specs = (P("tm", None, "space", None), P("tm", None, None, "space"), P(), P("tm", None))
    out_specs = (P("tm", None, None, "space", None), P("tm", None, None))
    return jax.shard_map(local, mesh=mesh, in_specs=in_specs, out_specs=out_specs, check_vma=False)
```

```python
import math

import jax
import jax.numpy as jnp
from jax import lax
from jax.experimental import pallas as pl
from jax.experimental.pallas import tpu as pltpu
from jax.sharding import PartitionSpec as P

EXTENT = 48
MOMS = 27
CHUNKS = 7
SIZE1, SIZE2 = 1.625, 1.1325
MESH = pl.DeviceIdType.MESH


def iota(shape, dim):
    return lax.broadcasted_iota(jnp.int32, shape, dim)


def swap_halves(array):
    return jnp.concatenate([array[:, 64:], array[:, :64]], axis=1)


def swapped(low, high, bit):
    has_bit = (iota((8, 128), 0) & bit) != 0
    return (
        jnp.where(has_bit, pltpu.roll(high, bit, 0), low),
        jnp.where(has_bit, high, pltpu.roll(low, 8 - bit, 0)),
    )


def fields_kernel(
    mom_h, pair_h, noise_h, vec_h, mesons, traces,
    mom_s, pair_s, spread, noise_v, vec_v, hrow, kap_r, kap_i,
    raw, core_in, half, y_in, own, z_in, slices, here, turned, four, eight,
    small_sem, noise_sem, vec_sem, core_s, core_r, y_s, y_r, z_s, z_r, t_s, t_r, four_s, four_r, eight_s, eight_r,
):
    space, tm = lax.axis_index("space"), lax.axis_index("tm")
    z, y, core = space // 4, lax.rem(space // 2, 2), lax.rem(space, 2)
    quad = lax.rem(space, 4)

    def in_z(d):
        return {"space": lax.rem(z + d, 8) * 4 + quad, "tm": tm}

    def in_quad(d):
        return {"space": z * 4 + (quad ^ d), "tm": tm}

    def in_tm(d):
        return {"space": space, "tm": lax.rem(tm + d, 8)}

    def load(tile):
        lanes = pl.ds(tile * 128, 128)
        return (
            pltpu.make_async_copy(noise_h.at[:, :, lanes], noise_v.at[tile], noise_sem.at[tile]),
            pltpu.make_async_copy(vec_h.at[:, lanes, :], vec_v.at[tile], vec_sem.at[tile]),
        )

    small = (
        pltpu.make_async_copy(mom_h, mom_s, small_sem.at[0]),
        pltpu.make_async_copy(pair_h, pair_s, small_sem.at[1]),
    )
    for copy in small:
        copy.start()
    for tile in range(4):
        for copy in load(tile):
            copy.start()

    barrier = pltpu.get_barrier_semaphore()
    for d in range(1, 4):
        pl.semaphore_signal(barrier, inc=1, device_id=in_quad(d), device_id_type=MESH)
    for d in range(1, 8):
        pl.semaphore_signal(barrier, inc=1, device_id=in_z(d), device_id_type=MESH)
        pl.semaphore_signal(barrier, inc=1, device_id=in_tm(d), device_id_type=MESH)

    for k in range(5):
        hrow[k, 0] = jnp.zeros((64, 128), jnp.float32)
        hrow[k, 11] = jnp.zeros((64, 128), jnp.float32)
    for copy in small:
        copy.wait()
    for q in range(MOMS):
        for k in range(3):
            spread[k, q : q + 1, :] = jnp.full((1, 128), mom_s[k, q], jnp.int32)

    scale = 1.0 / math.sqrt(12 * 512 * 32)
    row = space * 512 // EXTENT + iota((MOMS, 128), 1)
    q0 = jnp.abs(spread[0])
    angle = (spread[1] * lax.rem(row, EXTENT) + spread[2] * (row // EXTENT)).astype(jnp.float32)
    angle = angle * jnp.float32(2.0 * math.pi / EXTENT)
    size = jnp.where(q0 == 0, scale, jnp.where(q0 == 1, scale / SIZE1, scale / SIZE2))
    phase_r, phase_i = jnp.cos(angle) * size, -jnp.sin(angle) * size
    left = iota((MOMS, 128), 1) < 64
    for r in range(12):
        kap_r[r] = jnp.broadcast_to(phase_r[:, r : r + 1], (MOMS, 128))
        column = jnp.broadcast_to(phase_i[:, r : r + 1], (MOMS, 128))
        kap_i[r] = jnp.where(left, column, -column)

    phase0 = lax.rem(space * 32, EXTENT)
    lane = lax.rem(iota((8, 128), 1), 64)
    kind = iota((8, 128), 0)
    harmonic = jnp.where(kind < 2, 1, 2)
    amplitude = jnp.where(kind < 2, SIZE1, SIZE2)
    flip = jnp.where(iota((64, 128), 1) < 64, -1.0, 1.0).astype(jnp.bfloat16)

    def tile_step(tile, _):
        for copy in load(tile):
            copy.wait()
        starts = [phase0 + tile * 128 + 64 * h for h in range(2)]
        firsts = [lax.rem(start, EXTENT) for start in starts]
        waves = []
        for first in firsts:
            turn = ((first + lane) * harmonic).astype(jnp.float32) * jnp.float32(2.0 * math.pi / EXTENT)
            wave = amplitude * jnp.where(kind % 2 == 0, jnp.cos(turn), jnp.sin(turn))
            waves.append(wave.astype(jnp.bfloat16))
        totals = [None, None]
        for a4 in range(3):
            n = [noise_v[tile, 4 * a4 + a].astype(jnp.float32).astype(jnp.bfloat16) for a in range(4)]
            for h in range(2):
                cut = slice(64 * h, 64 * h + 64)
                joined = [jnp.concatenate([n[k][:, cut], n[k + 1][:, cut]], axis=1) for k in (0, 2)]
                n4 = jnp.concatenate(joined, axis=1)
                z4_r, z4_i = jnp.abs(n4 - 2) - 1, jnp.abs(n4 - 1) - 1
                wave = [jnp.concatenate([waves[h][k : k + 1, :]] * 2, axis=1) for k in range(4)]
                left_r = [z4_r, z4_r * wave[0], z4_i * -wave[1], z4_r * wave[2], z4_i * -wave[3]]
                left_i = [z4_i, z4_i * wave[0], z4_r * wave[1], z4_i * wave[2], z4_r * wave[3]]
                right_r, right_i = [], []
                for a in range(4):
                    v = vec_v[tile, 4 * a4 + a, 64 * h : 64 * h + 64, :]
                    t = swap_halves(v) * flip
                    for part, into in ((v, right_r), (t, right_i)):
                        for g in range(4):
                            piece = part[16 * g : 16 * g + 16]
                            zero = jnp.zeros_like(piece)
                            if g == 0:
                                pair = [piece, zero]
                            elif g == 3:
                                pair = [zero, piece]
                            else:
                                in_first = firsts[h] + 16 * g < EXTENT
                                pair = [jnp.where(in_first, piece, zero), jnp.where(in_first, zero, piece)]
                            into.append(jnp.concatenate(pair, axis=1))
                for lhs, rhs in ((left_r, right_r), (left_i, right_i)):
                    product = jnp.dot(
                        jnp.concatenate(lhs, axis=0), jnp.concatenate(rhs, axis=0), preferred_element_type=jnp.float32
                    )
                    totals[h] = product if totals[h] is None else totals[h] + product
        for h in range(2):
            f = [totals[h][64 * k : 64 * k + 64, :] for k in range(5)]
            terms = [f[3] + f[4], f[1] + f[2], f[0], f[1] - f[2], f[3] - f[4]]
            fresh = firsts[h] == 0 if h == 1 else (firsts[h] == 0) | (tile == 0)
            for k in range(5):
                at = starts[h] // EXTENT
                hrow[k, at] = jnp.where(fresh, 0.0, hrow[k, at]) + terms[k][:, 0:128]
                hrow[k, at + 1] = terms[k][:, 128:256]
        return 0

    lax.fori_loop(0, 4, tile_step, 0)
    pl.semaphore_wait(barrier, 17)

    def to_core(g):
        return pltpu.make_async_remote_copy(
            src_ref=raw.at[1 - core, g], dst_ref=core_in.at[g], send_sem=core_s.at[g], recv_sem=core_r.at[g],
            device_id=in_quad(1), device_id_type=MESH,
        )

    def to_y(g):
        return pltpu.make_async_remote_copy(
            src_ref=half.at[g, 1 - y], dst_ref=y_in.at[g], send_sem=y_s.at[g], recv_sem=y_r.at[g],
            device_id=in_quad(2), device_id_type=MESH,
        )

    def to_z(g, d):
        return pltpu.make_async_remote_copy(
            src_ref=own.at[g, lax.rem(z + d, 8)], dst_ref=z_in.at[g, d - 1],
            send_sem=z_s.at[g, d - 1], recv_sem=z_r.at[g, d - 1], device_id=in_z(d), device_id_type=MESH,
        )

    def to_tm(g, d):
        return pltpu.make_async_remote_copy(
            src_ref=slices.at[g, tm], dst_ref=slices.at[g, tm],
            send_sem=t_s.at[g, d - 1], recv_sem=t_r.at[g, d - 1], device_id=in_tm(d), device_id_type=MESH,
        )

    def momentum(g, k):
        q = lax.min(4 * g + k, MOMS - 1)
        q0 = mom_s[0, q] + 2
        acc_r = [jnp.zeros((8, 128), jnp.float32) for _ in range(8)]
        acc_i = [jnp.zeros((8, 128), jnp.float32) for _ in range(8)]
        for r in range(12):
            k_r = jnp.broadcast_to(kap_r[r, pl.ds(q, 1), :], (8, 128))
            k_i = jnp.broadcast_to(kap_i[r, pl.ds(q, 1), :], (8, 128))
            for i in range(8):
                part = hrow[q0, r, 8 * i : 8 * i + 8, :]
                acc_r[i] += k_r * part
                acc_i[i] += k_i * part
        tiles = [acc_r[i] + swap_halves(acc_i[i]) for i in range(8)]
        by_core = [swapped(tiles[2 * i], tiles[2 * i + 1], 2) for i in range(4)]
        for c in range(2):
            for i in range(2):
                by_y = swapped(by_core[2 * i][c], by_core[2 * i + 1][c], 4)
                for yy in range(2):
                    raw[c, g, yy, k, 8 * i : 8 * i + 8, :] = by_y[yy]

    def after_core(g):
        to_core(g).wait_recv()
        for yy in range(2):
            half[g, yy] = raw[core, g, yy] + core_in[g, yy]
        to_y(g).start()

    def first_step(g, _):
        for k in range(4):
            momentum(g, k)
        to_core(g).start()

        @pl.when(g >= 1)
        def _():
            after_core(g - 1)

        return 0

    lax.fori_loop(0, CHUNKS, first_step, 0)
    after_core(CHUNKS - 1)

    def after_y(g, _):
        to_y(g).wait_recv()
        sums = half[g, y] + y_in[g]
        for top in range(2):
            tiles = [sums[k, 8 * top : 8 * top + 8, :] for k in range(4)]
            low = [swapped(tiles[2 * k], tiles[2 * k + 1], 2) for k in range(2)]
            for bit in range(2):
                pair = swapped(low[0][bit], low[1][bit], 4)
                for upper in range(2):
                    own[g, 4 * top + 2 * upper + bit] = pair[upper]
        for d in range(1, 8):
            to_z(g, d).start()
        return 0

    lax.fori_loop(0, CHUNKS, after_y, 0)

    def after_z(g, _):
        total = own[g, z]
        for d in range(1, 8):
            to_z(g, d).wait_recv()
            total += z_in[g, d - 1]
        for k in range(4):
            for c in range(2):
                mesons[c, 4 * g + k] = total[2 * k : 2 * k + 2, 64 * c : 64 * c + 64]
        slices[g, tm] = total
        for d in range(1, 8):
            to_tm(g, d).start()
        return 0

    lax.fori_loop(0, CHUNKS, after_z, 0)

    lanes = iota((8, 128), 1)

    def after_tm(g, sums):
        for d in range(1, 8):
            to_tm(g, d).wait_recv()
        for t in range(8):
            tile = slices[g, t]
            here[t] = tile
            turned[t] = swap_halves(jnp.where(lanes < 64, tile, -tile))
        for k in range(8):
            sink, source, rotated = here[pair_s[1, k]], here[pair_s[0, k]], turned[pair_s[0, k]]
            for c, term in enumerate((sink * source, sink * rotated)):
                value = jnp.sum(term, axis=1, keepdims=True)
                sums = jnp.where(lanes == 16 * g + 2 * k + c, value, sums)
        return sums

    result = lax.fori_loop(0, CHUNKS, after_tm, jnp.zeros((8, 128), jnp.float32))
    result = result + pltpu.roll(result, 7, 0)
    for k in range(4):
        four[quad, k : k + 1, :] = result[2 * k : 2 * k + 1, :]

    def to_quad(d):
        return pltpu.make_async_remote_copy(
            src_ref=four.at[quad], dst_ref=four.at[quad], send_sem=four_s.at[d - 1], recv_sem=four_r.at[d - 1],
            device_id=in_quad(d), device_id_type=MESH,
        )

    def to_all_z(d):
        return pltpu.make_async_remote_copy(
            src_ref=eight.at[z], dst_ref=eight.at[z], send_sem=eight_s.at[d - 1], recv_sem=eight_r.at[d - 1],
            device_id=in_z(d), device_id_type=MESH,
        )

    for d in range(1, 4):
        to_quad(d).start()
    for d in range(1, 4):
        to_quad(d).wait_recv()
    eight[z] = (four[0] + four[1]) + (four[2] + four[3])
    for d in range(1, 8):
        to_all_z(d).start()
    for d in range(1, 8):
        to_all_z(d).wait_recv()
    total = eight[0]
    for k in range(1, 8):
        total += eight[k]
    columns = jnp.transpose(jnp.concatenate([total, total], axis=0) * (1.0 / 64))
    by_moment = jnp.concatenate([columns[16 * g : 16 * g + 16, 0:4] for g in range(CHUNKS)], axis=1)
    for k in range(8):
        traces[k] = by_moment[2 * k : 2 * k + 2, 0:MOMS]

    def finish(g, _):
        to_core(g).wait_send()
        to_y(g).wait_send()
        for d in range(1, 8):
            to_z(g, d).wait_send()
            to_tm(g, d).wait_send()
        return 0

    lax.fori_loop(0, CHUNKS, finish, 0)
    for d in range(1, 4):
        to_quad(d).wait_send()
    for d in range(1, 8):
        to_all_z(d).wait_send()


def write_kernel(mesons_v, traces_v, mesons_h, traces_h, sem):
    copies = (
        pltpu.make_async_copy(mesons_v.at[:, pl.ds(0, MOMS)], mesons_h, sem.at[0]),
        pltpu.make_async_copy(traces_v, traces_h, sem.at[1]),
    )
    for copy in copies:
        copy.start()
    for copy in copies:
        copy.wait()


def local(solutions, noise, momenta, pairs):
    f32, bf16 = jnp.float32, jnp.bfloat16
    vmem = pl.BlockSpec(memory_space=pltpu.VMEM)
    hbm = pl.BlockSpec(memory_space=pltpu.HBM)
    dma = pltpu.SemaphoreType.DMA
    mesons, traces = pl.pallas_call(
        fields_kernel,
        out_shape=(
            pltpu.VMEM((2, 4 * CHUNKS, 2, 64), f32),
            pltpu.VMEM((8, 2, MOMS), f32),
        ),
        in_specs=[hbm] * 4,
        out_specs=(vmem, vmem),
        scratch_shapes=[
            pltpu.SMEM((3, MOMS), jnp.int32),
            pltpu.SMEM((2, 8), jnp.int32),
            pltpu.VMEM((3, MOMS, 128), jnp.int32),
            pltpu.VMEM((4, 12, 64, 128), jnp.int32),
            pltpu.VMEM((4, 12, 128, 128), bf16),
            pltpu.VMEM((5, 12, 64, 128), f32),
            pltpu.VMEM((12, MOMS, 128), f32),
            pltpu.VMEM((12, MOMS, 128), f32),
            pltpu.VMEM((2, CHUNKS, 2, 4, 16, 128), f32),
            pltpu.VMEM((CHUNKS, 2, 4, 16, 128), f32),
            pltpu.VMEM((CHUNKS, 2, 4, 16, 128), f32),
            pltpu.VMEM((CHUNKS, 4, 16, 128), f32),
            pltpu.VMEM((CHUNKS, 8, 8, 128), f32),
            pltpu.VMEM((CHUNKS, 7, 8, 128), f32),
            pltpu.VMEM((CHUNKS, 8, 8, 128), f32),
            pltpu.VMEM((8, 8, 128), f32),
            pltpu.VMEM((8, 8, 128), f32),
            pltpu.VMEM((4, 4, 128), f32),
            pltpu.VMEM((8, 4, 128), f32),
            dma((2,)), dma((4,)), dma((4,)),
            dma((CHUNKS,)), dma((CHUNKS,)),
            dma((CHUNKS,)), dma((CHUNKS,)),
            dma((CHUNKS, 7)), dma((CHUNKS, 7)),
            dma((CHUNKS, 7)), dma((CHUNKS, 7)),
            dma((3,)), dma((3,)),
            dma((7,)), dma((7,)),
        ],
        compiler_params=pltpu.CompilerParams(
            collective_id=0, has_side_effects=True, vmem_limit_bytes=66700000
        ),
        name="meson_fields",
    )(momenta.T, pairs.T, noise[0].transpose(1, 0, 2), solutions[0])
    mesons, correlators = pl.pallas_call(
        write_kernel,
        out_shape=(
            jax.ShapeDtypeStruct((2, MOMS, 2, 64), f32),
            jax.ShapeDtypeStruct((8, 2, MOMS), f32),
        ),
        in_specs=[vmem] * 2,
        out_specs=(hbm, hbm),
        scratch_shapes=[dma((2,))],
        compiler_params=pltpu.CompilerParams(vmem_limit_bytes=1 << 20),
        name="write_out",
    )(mesons, traces)
    return (mesons[None], correlators)


def solution(mesh):
    in_specs = (P("tm", None, "space", None), P("tm", None, None, "space"), P(), P("tm", None))
    out_specs = (P("tm", None, None, "space", None), P("tm", None, None))
    return jax.shard_map(local, mesh=mesh, in_specs=in_specs, out_specs=out_specs, check_vma=False)
```

```python
import math

import jax
import jax.numpy as jnp
from jax import lax
from jax.experimental import pallas as pl
from jax.experimental.pallas import tpu as pltpu
from jax.sharding import PartitionSpec as P

EXTENT = 48
MOMS = 27
CHUNKS = 7
SIZE1, SIZE2 = 1.625, 1.1325
MESH = pl.DeviceIdType.MESH


def iota(shape, dim):
    return lax.broadcasted_iota(jnp.int32, shape, dim)


def swap_halves(array):
    return jnp.concatenate([array[:, 64:], array[:, :64]], axis=1)


def swapped(low, high, bit):
    has_bit = (iota((8, 128), 0) & bit) != 0
    return (
        jnp.where(has_bit, pltpu.roll(high, bit, 0), low),
        jnp.where(has_bit, high, pltpu.roll(low, 8 - bit, 0)),
    )


def fields_kernel(
    mom_h, pair_h, noise_h, vec_h, mesons, traces,
    mom_s, pair_s, spread, noise_v, vec_v, hrow, kap_r, kap_i,
    raw, core_in, half, y_in, own, z_in, slices, here, turned, both, chips,
    small_sem, noise_sem, vec_sem, core_s, core_r, y_s, y_r, z_s, z_r, t_s, t_r, last_s, last_r,
):
    space, tm = lax.axis_index("space"), lax.axis_index("tm")
    z, y, core = space // 4, lax.rem(space // 2, 2), lax.rem(space, 2)
    quad = lax.rem(space, 4)

    def in_z(d):
        return {"space": lax.rem(z + d, 8) * 4 + quad, "tm": tm}

    def in_quad(d):
        return {"space": z * 4 + (quad ^ d), "tm": tm}

    def in_chips(e, d):
        return {"space": (lax.rem(z + d, 8) * 4 + quad) ^ (2 * e), "tm": tm}

    def in_tm(d):
        return {"space": space, "tm": lax.rem(tm + d, 8)}

    def load(tile):
        lanes = pl.ds(tile * 128, 128)
        return (
            pltpu.make_async_copy(noise_h.at[:, :, lanes], noise_v.at[tile], noise_sem.at[tile]),
            pltpu.make_async_copy(vec_h.at[:, lanes, :], vec_v.at[tile], vec_sem.at[tile]),
        )

    small = (
        pltpu.make_async_copy(mom_h, mom_s, small_sem.at[0]),
        pltpu.make_async_copy(pair_h, pair_s, small_sem.at[1]),
    )
    for copy in small:
        copy.start()
    for tile in range(4):
        for copy in load(tile):
            copy.start()

    barrier = pltpu.get_barrier_semaphore()
    for d in range(1, 3):
        pl.semaphore_signal(barrier, inc=1, device_id=in_quad(d), device_id_type=MESH)
    for d in range(1, 8):
        pl.semaphore_signal(barrier, inc=1, device_id=in_z(d), device_id_type=MESH)
        pl.semaphore_signal(barrier, inc=1, device_id=in_tm(d), device_id_type=MESH)

    for k in range(5):
        hrow[k, 0] = jnp.zeros((64, 128), jnp.float32)
        hrow[k, 11] = jnp.zeros((64, 128), jnp.float32)
    for copy in small:
        copy.wait()
    for q in range(MOMS):
        for k in range(3):
            spread[k, q : q + 1, :] = jnp.full((1, 128), mom_s[k, q], jnp.int32)

    scale = 1.0 / math.sqrt(12 * 512 * 32)
    row = space * 512 // EXTENT + iota((MOMS, 128), 1)
    q0 = jnp.abs(spread[0])
    angle = (spread[1] * lax.rem(row, EXTENT) + spread[2] * (row // EXTENT)).astype(jnp.float32)
    angle = angle * jnp.float32(2.0 * math.pi / EXTENT)
    size = jnp.where(q0 == 0, scale, jnp.where(q0 == 1, scale / SIZE1, scale / SIZE2))
    phase_r, phase_i = jnp.cos(angle) * size, -jnp.sin(angle) * size
    left = iota((MOMS, 128), 1) < 64
    for r in range(12):
        kap_r[r] = jnp.broadcast_to(phase_r[:, r : r + 1], (MOMS, 128))
        column = jnp.broadcast_to(phase_i[:, r : r + 1], (MOMS, 128))
        kap_i[r] = jnp.where(left, column, -column)

    phase0 = lax.rem(space * 32, EXTENT)
    lane = lax.rem(iota((8, 128), 1), 64)
    kind = iota((8, 128), 0)
    harmonic = jnp.where(kind < 2, 1, 2)
    amplitude = jnp.where(kind < 2, SIZE1, SIZE2)
    flip = jnp.where(iota((64, 128), 1) < 64, -1.0, 1.0).astype(jnp.bfloat16)

    def tile_step(tile, _):
        for copy in load(tile):
            copy.wait()
        starts = [phase0 + tile * 128 + 64 * h for h in range(2)]
        firsts = [lax.rem(start, EXTENT) for start in starts]
        waves = []
        for first in firsts:
            turn = ((first + lane) * harmonic).astype(jnp.float32) * jnp.float32(2.0 * math.pi / EXTENT)
            wave = amplitude * jnp.where(kind % 2 == 0, jnp.cos(turn), jnp.sin(turn))
            waves.append(wave.astype(jnp.bfloat16))
        totals = [None, None]
        for a4 in range(3):
            n = [noise_v[tile, 4 * a4 + a].astype(jnp.float32).astype(jnp.bfloat16) for a in range(4)]
            for h in range(2):
                cut = slice(64 * h, 64 * h + 64)
                joined = [jnp.concatenate([n[k][:, cut], n[k + 1][:, cut]], axis=1) for k in (0, 2)]
                n4 = jnp.concatenate(joined, axis=1)
                z4_r, z4_i = jnp.abs(n4 - 2) - 1, jnp.abs(n4 - 1) - 1
                wave = [jnp.concatenate([waves[h][k : k + 1, :]] * 2, axis=1) for k in range(4)]
                left_r = [z4_r, z4_r * wave[0], z4_i * -wave[1], z4_r * wave[2], z4_i * -wave[3]]
                left_i = [z4_i, z4_i * wave[0], z4_r * wave[1], z4_i * wave[2], z4_r * wave[3]]
                right_r, right_i = [], []
                for a in range(4):
                    v = vec_v[tile, 4 * a4 + a, 64 * h : 64 * h + 64, :]
                    t = swap_halves(v) * flip
                    for part, into in ((v, right_r), (t, right_i)):
                        for g in range(4):
                            piece = part[16 * g : 16 * g + 16]
                            zero = jnp.zeros_like(piece)
                            if g == 0:
                                pair = [piece, zero]
                            elif g == 3:
                                pair = [zero, piece]
                            else:
                                in_first = firsts[h] + 16 * g < EXTENT
                                pair = [jnp.where(in_first, piece, zero), jnp.where(in_first, zero, piece)]
                            into.append(jnp.concatenate(pair, axis=1))
                for lhs, rhs in ((left_r, right_r), (left_i, right_i)):
                    product = jnp.dot(
                        jnp.concatenate(lhs, axis=0), jnp.concatenate(rhs, axis=0), preferred_element_type=jnp.float32
                    )
                    totals[h] = product if totals[h] is None else totals[h] + product
        for h in range(2):
            f = [totals[h][64 * k : 64 * k + 64, :] for k in range(5)]
            terms = [f[3] + f[4], f[1] + f[2], f[0], f[1] - f[2], f[3] - f[4]]
            fresh = firsts[h] == 0 if h == 1 else (firsts[h] == 0) | (tile == 0)
            for k in range(5):
                at = starts[h] // EXTENT
                hrow[k, at] = jnp.where(fresh, 0.0, hrow[k, at]) + terms[k][:, 0:128]
                hrow[k, at + 1] = terms[k][:, 128:256]
        return 0

    lax.fori_loop(0, 4, tile_step, 0)
    pl.semaphore_wait(barrier, 16)

    def to_core(g):
        return pltpu.make_async_remote_copy(
            src_ref=raw.at[1 - core, g], dst_ref=core_in.at[g], send_sem=core_s.at[0], recv_sem=core_r.at[g],
            device_id=in_quad(1), device_id_type=MESH,
        )

    def to_y(g):
        return pltpu.make_async_remote_copy(
            src_ref=half.at[g, 1 - y], dst_ref=y_in.at[g], send_sem=y_s.at[0], recv_sem=y_r.at[g],
            device_id=in_quad(2), device_id_type=MESH,
        )

    def to_z(g, d):
        return pltpu.make_async_remote_copy(
            src_ref=own.at[g, lax.rem(z + d, 8)], dst_ref=z_in.at[g, d - 1],
            send_sem=z_s.at[0], recv_sem=z_r.at[g], device_id=in_z(d), device_id_type=MESH,
        )

    def to_tm(g, d):
        return pltpu.make_async_remote_copy(
            src_ref=slices.at[g, tm], dst_ref=slices.at[g, tm],
            send_sem=t_s.at[0], recv_sem=t_r.at[g], device_id=in_tm(d), device_id_type=MESH,
        )

    def arrive(ref, sem):
        pltpu.make_async_copy(ref, ref, sem).wait()

    def momentum(g, k):
        q = lax.min(4 * g + k, MOMS - 1)
        q0 = mom_s[0, q] + 2
        acc_r = [jnp.zeros((8, 128), jnp.float32) for _ in range(8)]
        acc_i = [jnp.zeros((8, 128), jnp.float32) for _ in range(8)]
        for r in range(12):
            k_r = jnp.broadcast_to(kap_r[r, pl.ds(q, 1), :], (8, 128))
            k_i = jnp.broadcast_to(kap_i[r, pl.ds(q, 1), :], (8, 128))
            for i in range(8):
                part = hrow[q0, r, 8 * i : 8 * i + 8, :]
                acc_r[i] += k_r * part
                acc_i[i] += k_i * part
        tiles = [acc_r[i] + swap_halves(acc_i[i]) for i in range(8)]
        by_core = [swapped(tiles[2 * i], tiles[2 * i + 1], 2) for i in range(4)]
        for c in range(2):
            for i in range(2):
                by_y = swapped(by_core[2 * i][c], by_core[2 * i + 1][c], 4)
                for yy in range(2):
                    raw[c, g, yy, k, 8 * i : 8 * i + 8, :] = by_y[yy]

    def after_core(g):
        to_core(g).wait_recv()
        for yy in range(2):
            half[g, yy] = raw[core, g, yy] + core_in[g, yy]
        to_y(g).start()

    def first_step(g, _):
        for k in range(4):
            momentum(g, k)
        to_core(g).start()

        @pl.when(g >= 1)
        def _():
            after_core(g - 1)

        return 0

    lax.fori_loop(0, CHUNKS, first_step, 0)
    after_core(CHUNKS - 1)

    def after_y(g, _):
        to_y(g).wait_recv()
        sums = half[g, y] + y_in[g]
        for top in range(2):
            tiles = [sums[k, 8 * top : 8 * top + 8, :] for k in range(4)]
            low = [swapped(tiles[2 * k], tiles[2 * k + 1], 2) for k in range(2)]
            for bit in range(2):
                pair = swapped(low[0][bit], low[1][bit], 4)
                for upper in range(2):
                    own[g, 4 * top + 2 * upper + bit] = pair[upper]
        for d in range(1, 8):
            to_z(g, d).start()
        return 0

    lax.fori_loop(0, CHUNKS, after_y, 0)

    def after_z(g, _):
        arrive(z_in.at[g], z_r.at[g])
        total = own[g, z]
        for d in range(7):
            total += z_in[g, d]
        for k in range(4):
            for c in range(2):
                mesons[c, 4 * g + k] = total[2 * k : 2 * k + 2, 64 * c : 64 * c + 64]
        slices[g, tm] = total
        for d in range(1, 8):
            to_tm(g, d).start()
        return 0

    lax.fori_loop(0, CHUNKS, after_z, 0)

    lanes = iota((8, 128), 1)

    def after_tm(g, sums):
        arrive(slices.at[g, pl.ds(0, 7)], t_r.at[g])
        for t in range(8):
            tile = slices[g, t]
            here[t] = tile
            turned[t] = swap_halves(jnp.where(lanes < 64, tile, -tile))
        for k in range(8):
            sink, source, rotated = here[pair_s[1, k]], here[pair_s[0, k]], turned[pair_s[0, k]]
            for c, term in enumerate((sink * source, sink * rotated)):
                value = jnp.sum(term, axis=1, keepdims=True)
                sums = jnp.where(lanes == 16 * g + 2 * k + c, value, sums)
        return sums

    result = lax.fori_loop(0, CHUNKS, after_tm, jnp.zeros((8, 128), jnp.float32))
    result = result + pltpu.roll(result, 7, 0)
    for k in range(4):
        both[core, k : k + 1, :] = result[2 * k : 2 * k + 1, :]
    to_other = pltpu.make_async_remote_copy(
        src_ref=both.at[core], dst_ref=both.at[core], send_sem=last_s.at[0], recv_sem=last_r.at[0],
        device_id=in_quad(1), device_id_type=MESH,
    )
    chip = z * 2 + y

    def to_chip(e, d):
        return pltpu.make_async_remote_copy(
            src_ref=chips.at[chip], dst_ref=chips.at[chip], send_sem=last_s.at[1], recv_sem=last_r.at[1],
            device_id=in_chips(e, d), device_id_type=MESH,
        )

    to_other.start()
    to_other.wait_recv()
    chips[chip] = both[0] + both[1]
    for e in range(2):
        for d in range(1 - e, 8):
            to_chip(e, d).start()
    arrive(chips.at[pl.ds(0, 15)], last_r.at[1])
    total = chips[0]
    for k in range(1, 16):
        total += chips[k]
    columns = jnp.transpose(jnp.concatenate([total, total], axis=0) * (1.0 / 64))
    by_moment = jnp.concatenate([columns[16 * g : 16 * g + 16, 0:4] for g in range(CHUNKS)], axis=1)
    for k in range(8):
        traces[k] = by_moment[2 * k : 2 * k + 2, 0:MOMS]

    arrive(raw.at[0], core_s.at[0])
    arrive(y_in, y_s.at[0])
    arrive(z_in, z_s.at[0])
    arrive(slices.at[:, pl.ds(0, 7)], t_s.at[0])
    to_other.wait_send()
    arrive(chips.at[pl.ds(0, 15)], last_s.at[1])


def write_kernel(mesons_v, traces_v, mesons_h, traces_h, sem):
    copies = (
        pltpu.make_async_copy(mesons_v.at[:, pl.ds(0, MOMS)], mesons_h, sem.at[0]),
        pltpu.make_async_copy(traces_v, traces_h, sem.at[1]),
    )
    for copy in copies:
        copy.start()
    for copy in copies:
        copy.wait()


def local(solutions, noise, momenta, pairs):
    f32, bf16 = jnp.float32, jnp.bfloat16
    vmem = pl.BlockSpec(memory_space=pltpu.VMEM)
    hbm = pl.BlockSpec(memory_space=pltpu.HBM)
    dma = pltpu.SemaphoreType.DMA
    mesons, traces = pl.pallas_call(
        fields_kernel,
        out_shape=(
            pltpu.VMEM((2, 4 * CHUNKS, 2, 64), f32),
            pltpu.VMEM((8, 2, MOMS), f32),
        ),
        in_specs=[hbm] * 4,
        out_specs=(vmem, vmem),
        scratch_shapes=[
            pltpu.SMEM((3, MOMS), jnp.int32),
            pltpu.SMEM((2, 8), jnp.int32),
            pltpu.VMEM((3, MOMS, 128), jnp.int32),
            pltpu.VMEM((4, 12, 64, 128), jnp.int32),
            pltpu.VMEM((4, 12, 128, 128), bf16),
            pltpu.VMEM((5, 12, 64, 128), f32),
            pltpu.VMEM((12, MOMS, 128), f32),
            pltpu.VMEM((12, MOMS, 128), f32),
            pltpu.VMEM((2, CHUNKS, 2, 4, 16, 128), f32),
            pltpu.VMEM((CHUNKS, 2, 4, 16, 128), f32),
            pltpu.VMEM((CHUNKS, 2, 4, 16, 128), f32),
            pltpu.VMEM((CHUNKS, 4, 16, 128), f32),
            pltpu.VMEM((CHUNKS, 8, 8, 128), f32),
            pltpu.VMEM((CHUNKS, 7, 8, 128), f32),
            pltpu.VMEM((CHUNKS, 8, 8, 128), f32),
            pltpu.VMEM((8, 8, 128), f32),
            pltpu.VMEM((8, 8, 128), f32),
            pltpu.VMEM((2, 4, 128), f32),
            pltpu.VMEM((16, 4, 128), f32),
            dma((2,)), dma((4,)), dma((4,)),
            dma((1,)), dma((CHUNKS,)),
            dma((1,)), dma((CHUNKS,)),
            dma((1,)), dma((CHUNKS,)),
            dma((1,)), dma((CHUNKS,)),
            dma((2,)), dma((2,)),
        ],
        compiler_params=pltpu.CompilerParams(
            collective_id=0, has_side_effects=True, vmem_limit_bytes=66700000
        ),
        name="meson_fields",
    )(momenta.T, pairs.T, noise[0].transpose(1, 0, 2), solutions[0])
    mesons, correlators = pl.pallas_call(
        write_kernel,
        out_shape=(
            jax.ShapeDtypeStruct((2, MOMS, 2, 64), f32),
            jax.ShapeDtypeStruct((8, 2, MOMS), f32),
        ),
        in_specs=[vmem] * 2,
        out_specs=(hbm, hbm),
        scratch_shapes=[dma((2,))],
        compiler_params=pltpu.CompilerParams(vmem_limit_bytes=1 << 20),
        name="write_out",
    )(mesons, traces)
    return (mesons[None], correlators)


def solution(mesh):
    in_specs = (P("tm", None, "space", None), P("tm", None, None, "space"), P(), P("tm", None))
    out_specs = (P("tm", None, None, "space", None), P("tm", None, None))
    return jax.shard_map(local, mesh=mesh, in_specs=in_specs, out_specs=out_specs, check_vma=False)
```

```python
import math

import jax
import jax.numpy as jnp
from jax import lax
from jax.experimental import pallas as pl
from jax.experimental.pallas import tpu as pltpu
from jax.sharding import PartitionSpec as P

EXTENT = 48
MOMS = 27
CHUNKS = 7
SIZE1, SIZE2 = 1.625, 1.1325
MESH = pl.DeviceIdType.MESH
OTHERS = [(e, d) for e in range(2) for d in range(8) if (e, d) != (0, 0)]


def iota(shape, dim):
    return lax.broadcasted_iota(jnp.int32, shape, dim)


def swap_halves(array):
    return jnp.concatenate([array[:, 64:], array[:, :64]], axis=1)


def swapped(low, high, bit):
    has_bit = (iota((8, 128), 0) & bit) != 0
    return (
        jnp.where(has_bit, pltpu.roll(high, bit, 0), low),
        jnp.where(has_bit, high, pltpu.roll(low, 8 - bit, 0)),
    )


def fields_kernel(
    mom_h, pair_h, noise_h, vec_h, mesons, traces,
    mom_s, pair_s, spread, noise_v, vec_v, hrow, kap_r, kap_i,
    raw, core_in, half, y_in, own, z_in, slices, here, turned, chips,
    small_sem, noise_sem, vec_sem, core_s, core_r, y_s, y_r, z_s, z_r, t_s, t_r, last_s, last_r,
):
    space, tm = lax.axis_index("space"), lax.axis_index("tm")
    z, y, core = space // 4, lax.rem(space // 2, 2), lax.rem(space, 2)
    quad = lax.rem(space, 4)

    def in_z(d):
        return {"space": lax.rem(z + d, 8) * 4 + quad, "tm": tm}

    def in_quad(d):
        return {"space": z * 4 + (quad ^ d), "tm": tm}

    def in_chips(e, d):
        return {"space": (lax.rem(z + d, 8) * 4 + quad) ^ (2 * e), "tm": tm}

    def in_tm(e, d):
        return {"space": space ^ e, "tm": lax.rem(tm + d, 8)}

    def load(tile):
        lanes = pl.ds(tile * 128, 128)
        return (
            pltpu.make_async_copy(noise_h.at[:, :, lanes], noise_v.at[tile], noise_sem.at[tile]),
            pltpu.make_async_copy(vec_h.at[:, lanes, :], vec_v.at[tile], vec_sem.at[tile]),
        )

    small = (
        pltpu.make_async_copy(mom_h, mom_s, small_sem.at[0]),
        pltpu.make_async_copy(pair_h, pair_s, small_sem.at[1]),
    )
    for copy in small:
        copy.start()
    for tile in range(4):
        for copy in load(tile):
            copy.start()

    barrier = pltpu.get_barrier_semaphore()
    for d in range(1, 3):
        pl.semaphore_signal(barrier, inc=1, device_id=in_quad(d), device_id_type=MESH)
    for d in range(1, 8):
        pl.semaphore_signal(barrier, inc=1, device_id=in_z(d), device_id_type=MESH)
        pl.semaphore_signal(barrier, inc=1, device_id=in_tm(0, d), device_id_type=MESH)

    for k in range(5):
        hrow[k, 0] = jnp.zeros((64, 128), jnp.float32)
        hrow[k, 11] = jnp.zeros((64, 128), jnp.float32)
    for copy in small:
        copy.wait()
    for q in range(MOMS):
        for k in range(3):
            spread[k, q : q + 1, :] = jnp.full((1, 128), mom_s[k, q], jnp.int32)

    scale = 1.0 / math.sqrt(12 * 512 * 32)
    row = space * 512 // EXTENT + iota((MOMS, 128), 1)
    q0 = jnp.abs(spread[0])
    angle = (spread[1] * lax.rem(row, EXTENT) + spread[2] * (row // EXTENT)).astype(jnp.float32)
    angle = angle * jnp.float32(2.0 * math.pi / EXTENT)
    size = jnp.where(q0 == 0, scale, jnp.where(q0 == 1, scale / SIZE1, scale / SIZE2))
    phase_r, phase_i = jnp.cos(angle) * size, -jnp.sin(angle) * size
    left = iota((MOMS, 128), 1) < 64
    for r in range(12):
        kap_r[r] = jnp.broadcast_to(phase_r[:, r : r + 1], (MOMS, 128))
        column = jnp.broadcast_to(phase_i[:, r : r + 1], (MOMS, 128))
        kap_i[r] = jnp.where(left, column, -column)

    phase0 = lax.rem(space * 32, EXTENT)
    lane = lax.rem(iota((8, 128), 1), 64)
    kind = iota((8, 128), 0)
    harmonic = jnp.where(kind < 2, 1, 2)
    amplitude = jnp.where(kind < 2, SIZE1, SIZE2)
    flip = jnp.where(iota((64, 128), 1) < 64, -1.0, 1.0).astype(jnp.bfloat16)

    def tile_step(tile, _):
        for copy in load(tile):
            copy.wait()
        starts = [phase0 + tile * 128 + 64 * h for h in range(2)]
        firsts = [lax.rem(start, EXTENT) for start in starts]
        waves = []
        for first in firsts:
            turn = ((first + lane) * harmonic).astype(jnp.float32) * jnp.float32(2.0 * math.pi / EXTENT)
            wave = amplitude * jnp.where(kind % 2 == 0, jnp.cos(turn), jnp.sin(turn))
            waves.append(wave.astype(jnp.bfloat16))
        totals = [None, None]
        for a4 in range(3):
            n = [noise_v[tile, 4 * a4 + a].astype(jnp.float32).astype(jnp.bfloat16) for a in range(4)]
            for h in range(2):
                cut = slice(64 * h, 64 * h + 64)
                joined = [jnp.concatenate([n[k][:, cut], n[k + 1][:, cut]], axis=1) for k in (0, 2)]
                n4 = jnp.concatenate(joined, axis=1)
                z4_r, z4_i = jnp.abs(n4 - 2) - 1, jnp.abs(n4 - 1) - 1
                wave = [jnp.concatenate([waves[h][k : k + 1, :]] * 2, axis=1) for k in range(4)]
                left_r = [z4_r, z4_r * wave[0], z4_i * -wave[1], z4_r * wave[2], z4_i * -wave[3]]
                left_i = [z4_i, z4_i * wave[0], z4_r * wave[1], z4_i * wave[2], z4_r * wave[3]]
                right_r, right_i = [], []
                for a in range(4):
                    v = vec_v[tile, 4 * a4 + a, 64 * h : 64 * h + 64, :]
                    t = swap_halves(v) * flip
                    for part, into in ((v, right_r), (t, right_i)):
                        for g in range(4):
                            piece = part[16 * g : 16 * g + 16]
                            zero = jnp.zeros_like(piece)
                            if g == 0:
                                pair = [piece, zero]
                            elif g == 3:
                                pair = [zero, piece]
                            else:
                                in_first = firsts[h] + 16 * g < EXTENT
                                pair = [jnp.where(in_first, piece, zero), jnp.where(in_first, zero, piece)]
                            into.append(jnp.concatenate(pair, axis=1))
                for lhs, rhs in ((left_r, right_r), (left_i, right_i)):
                    product = jnp.dot(
                        jnp.concatenate(lhs, axis=0), jnp.concatenate(rhs, axis=0), preferred_element_type=jnp.float32
                    )
                    totals[h] = product if totals[h] is None else totals[h] + product
        for h in range(2):
            f = [totals[h][64 * k : 64 * k + 64, :] for k in range(5)]
            terms = [f[3] + f[4], f[1] + f[2], f[0], f[1] - f[2], f[3] - f[4]]
            fresh = firsts[h] == 0 if h == 1 else (firsts[h] == 0) | (tile == 0)
            for k in range(5):
                at = starts[h] // EXTENT
                hrow[k, at] = jnp.where(fresh, 0.0, hrow[k, at]) + terms[k][:, 0:128]
                hrow[k, at + 1] = terms[k][:, 128:256]
        return 0

    lax.fori_loop(0, 4, tile_step, 0)
    pl.semaphore_wait(barrier, 16)

    def to_core(g):
        return pltpu.make_async_remote_copy(
            src_ref=raw.at[1 - core, g], dst_ref=core_in.at[g], send_sem=core_s.at[0], recv_sem=core_r.at[g],
            device_id=in_quad(1), device_id_type=MESH,
        )

    def to_y(g):
        return pltpu.make_async_remote_copy(
            src_ref=half.at[g, 1 - y], dst_ref=y_in.at[g], send_sem=y_s.at[0], recv_sem=y_r.at[g],
            device_id=in_quad(2), device_id_type=MESH,
        )

    def to_z(g, d):
        return pltpu.make_async_remote_copy(
            src_ref=own.at[g, lax.rem(z + d, 8)], dst_ref=z_in.at[g, d - 1],
            send_sem=z_s.at[0], recv_sem=z_r.at[g], device_id=in_z(d), device_id_type=MESH,
        )

    mine = core * 8 + tm

    def to_tm(g, e, d):
        return pltpu.make_async_remote_copy(
            src_ref=slices.at[g, mine], dst_ref=slices.at[g, mine],
            send_sem=t_s.at[0], recv_sem=t_r.at[g], device_id=in_tm(e, d), device_id_type=MESH,
        )

    def arrive(ref, sem):
        pltpu.make_async_copy(ref, ref, sem).wait()

    def momentum(g, k):
        q = lax.min(4 * g + k, MOMS - 1)
        q0 = mom_s[0, q] + 2
        acc_r = [jnp.zeros((8, 128), jnp.float32) for _ in range(8)]
        acc_i = [jnp.zeros((8, 128), jnp.float32) for _ in range(8)]
        for r in range(12):
            k_r = jnp.broadcast_to(kap_r[r, pl.ds(q, 1), :], (8, 128))
            k_i = jnp.broadcast_to(kap_i[r, pl.ds(q, 1), :], (8, 128))
            for i in range(8):
                part = hrow[q0, r, 8 * i : 8 * i + 8, :]
                acc_r[i] += k_r * part
                acc_i[i] += k_i * part
        tiles = [acc_r[i] + swap_halves(acc_i[i]) for i in range(8)]
        by_core = [swapped(tiles[2 * i], tiles[2 * i + 1], 2) for i in range(4)]
        for c in range(2):
            for i in range(2):
                by_y = swapped(by_core[2 * i][c], by_core[2 * i + 1][c], 4)
                for yy in range(2):
                    raw[c, g, yy, k, 8 * i : 8 * i + 8, :] = by_y[yy]

    def after_core(g):
        to_core(g).wait_recv()
        for yy in range(2):
            half[g, yy] = raw[core, g, yy] + core_in[g, yy]
        to_y(g).start()

    def first_step(g, _):
        for k in range(4):
            momentum(g, k)
        to_core(g).start()

        @pl.when(g >= 1)
        def _():
            after_core(g - 1)

        return 0

    lax.fori_loop(0, CHUNKS, first_step, 0)
    after_core(CHUNKS - 1)

    def after_y(g, _):
        to_y(g).wait_recv()
        sums = half[g, y] + y_in[g]
        for top in range(2):
            tiles = [sums[k, 8 * top : 8 * top + 8, :] for k in range(4)]
            low = [swapped(tiles[2 * k], tiles[2 * k + 1], 2) for k in range(2)]
            for bit in range(2):
                pair = swapped(low[0][bit], low[1][bit], 4)
                for upper in range(2):
                    own[g, 4 * top + 2 * upper + bit] = pair[upper]
        for d in range(1, 8):
            to_z(g, d).start()
        return 0

    lax.fori_loop(0, CHUNKS, after_y, 0)

    def after_z(g, _):
        arrive(z_in.at[g], z_r.at[g])
        total = own[g, z]
        for d in range(7):
            total += z_in[g, d]
        for k in range(4):
            for c in range(2):
                mesons[c, 4 * g + k] = total[2 * k : 2 * k + 2, 64 * c : 64 * c + 64]
        slices[g, mine] = total
        for e, d in OTHERS:
            to_tm(g, e, d).start()
        return 0

    lax.fori_loop(0, CHUNKS, after_z, 0)

    lanes = iota((8, 128), 1)

    def after_tm(g, sums):
        arrive(slices.at[g, pl.ds(0, 15)], t_r.at[g])
        for c in range(2):
            for t in range(8):
                tile = slices[g, 8 * c + t]
                here[t, c] = tile
                turned[t, c] = swap_halves(jnp.where(lanes < 64, tile, -tile))
        for k in range(8):
            sink, source, rotated = here[pair_s[1, k]], here[pair_s[0, k]], turned[pair_s[0, k]]
            for c, term in enumerate((sink * source, sink * rotated)):
                value = jnp.sum(term[0] + term[1], axis=1, keepdims=True)
                sums = jnp.where(lanes == 16 * g + 2 * k + c, value, sums)
        return sums

    result = lax.fori_loop(0, CHUNKS, after_tm, jnp.zeros((8, 128), jnp.float32))
    result = result + pltpu.roll(result, 7, 0)
    chip = z * 2 + y

    def to_chip(e, d):
        return pltpu.make_async_remote_copy(
            src_ref=chips.at[chip], dst_ref=chips.at[chip], send_sem=last_s.at[0], recv_sem=last_r.at[0],
            device_id=in_chips(e, d), device_id_type=MESH,
        )

    for k in range(4):
        chips[chip, k : k + 1, :] = result[2 * k : 2 * k + 1, :]
    for e, d in OTHERS:
        to_chip(e, d).start()
    arrive(chips.at[pl.ds(0, 15)], last_r.at[0])
    total = chips[0]
    for k in range(1, 16):
        total += chips[k]
    columns = jnp.transpose(jnp.concatenate([total, total], axis=0) * (1.0 / 64))
    by_moment = jnp.concatenate([columns[16 * g : 16 * g + 16, 0:4] for g in range(CHUNKS)], axis=1)
    for k in range(8):
        traces[k] = by_moment[2 * k : 2 * k + 2, 0:MOMS]

    arrive(raw.at[0], core_s.at[0])
    arrive(y_in, y_s.at[0])
    arrive(z_in, z_s.at[0])
    arrive(slices.at[:, pl.ds(0, 15)], t_s.at[0])
    arrive(chips.at[pl.ds(0, 15)], last_s.at[0])


def write_kernel(mesons_v, traces_v, mesons_h, traces_h, sem):
    copies = (
        pltpu.make_async_copy(mesons_v.at[:, pl.ds(0, MOMS)], mesons_h, sem.at[0]),
        pltpu.make_async_copy(traces_v, traces_h, sem.at[1]),
    )
    for copy in copies:
        copy.start()
    for copy in copies:
        copy.wait()


def local(solutions, noise, momenta, pairs):
    f32, bf16 = jnp.float32, jnp.bfloat16
    vmem = pl.BlockSpec(memory_space=pltpu.VMEM)
    hbm = pl.BlockSpec(memory_space=pltpu.HBM)
    dma = pltpu.SemaphoreType.DMA
    mesons, traces = pl.pallas_call(
        fields_kernel,
        out_shape=(
            pltpu.VMEM((2, 4 * CHUNKS, 2, 64), f32),
            pltpu.VMEM((8, 2, MOMS), f32),
        ),
        in_specs=[hbm] * 4,
        out_specs=(vmem, vmem),
        scratch_shapes=[
            pltpu.SMEM((3, MOMS), jnp.int32),
            pltpu.SMEM((2, 8), jnp.int32),
            pltpu.VMEM((3, MOMS, 128), jnp.int32),
            pltpu.VMEM((4, 12, 64, 128), jnp.int32),
            pltpu.VMEM((4, 12, 128, 128), bf16),
            pltpu.VMEM((5, 12, 64, 128), f32),
            pltpu.VMEM((12, MOMS, 128), f32),
            pltpu.VMEM((12, MOMS, 128), f32),
            pltpu.VMEM((2, CHUNKS, 2, 4, 16, 128), f32),
            pltpu.VMEM((CHUNKS, 2, 4, 16, 128), f32),
            pltpu.VMEM((CHUNKS, 2, 4, 16, 128), f32),
            pltpu.VMEM((CHUNKS, 4, 16, 128), f32),
            pltpu.VMEM((CHUNKS, 8, 8, 128), f32),
            pltpu.VMEM((CHUNKS, 7, 8, 128), f32),
            pltpu.VMEM((CHUNKS, 16, 8, 128), f32),
            pltpu.VMEM((8, 2, 8, 128), f32),
            pltpu.VMEM((8, 2, 8, 128), f32),
            pltpu.VMEM((16, 4, 128), f32),
            dma((2,)), dma((4,)), dma((4,)),
            dma((1,)), dma((CHUNKS,)),
            dma((1,)), dma((CHUNKS,)),
            dma((1,)), dma((CHUNKS,)),
            dma((1,)), dma((CHUNKS,)),
            dma((1,)), dma((1,)),
        ],
        compiler_params=pltpu.CompilerParams(
            collective_id=0, has_side_effects=True, vmem_limit_bytes=66700000
        ),
        name="meson_fields",
    )(momenta.T, pairs.T, noise[0].transpose(1, 0, 2), solutions[0])
    mesons, correlators = pl.pallas_call(
        write_kernel,
        out_shape=(
            jax.ShapeDtypeStruct((2, MOMS, 2, 64), f32),
            jax.ShapeDtypeStruct((8, 2, MOMS), f32),
        ),
        in_specs=[vmem] * 2,
        out_specs=(hbm, hbm),
        scratch_shapes=[dma((2,))],
        compiler_params=pltpu.CompilerParams(vmem_limit_bytes=1 << 20),
        name="write_out",
    )(mesons, traces)
    return (mesons[None], correlators)


def solution(mesh):
    in_specs = (P("tm", None, "space", None), P("tm", None, None, "space"), P(), P("tm", None))
    out_specs = (P("tm", None, None, "space", None), P("tm", None, None))
    return jax.shard_map(local, mesh=mesh, in_specs=in_specs, out_specs=out_specs, check_vma=False)
```

```python
import math

import jax
import jax.numpy as jnp
from jax import lax
from jax.experimental import pallas as pl
from jax.experimental.pallas import tpu as pltpu
from jax.sharding import PartitionSpec as P

EXTENT = 48
MOMS = 27
CHUNKS = 7
LAG = 1
SIZE1, SIZE2 = 1.625, 1.1325
MESH = pl.DeviceIdType.MESH
FAR_FIRST = (4, 3, 5, 2, 6, 1, 7)
OTHERS = [(e, d) for d in FAR_FIRST for e in (1, 0)] + [(1, 0)]


def iota(shape, dim):
    return lax.broadcasted_iota(jnp.int32, shape, dim)


def swap_halves(array):
    return jnp.concatenate([array[:, 64:], array[:, :64]], axis=1)


def swapped(low, high, bit):
    has_bit = (iota((8, 128), 0) & bit) != 0
    return (
        jnp.where(has_bit, pltpu.roll(high, bit, 0), low),
        jnp.where(has_bit, high, pltpu.roll(low, 8 - bit, 0)),
    )


def fields_kernel(
    mom_h, pair_h, noise_h, vec_h, mesons, traces,
    mom_s, pair_s, spread, noise_v, vec_v, hrow, kap_r, kap_i,
    raw, core_in, half, y_in, own, z_in, slices, here, turned, chips,
    small_sem, noise_sem, vec_sem, core_s, core_r, y_s, y_r, z_s, z_r, t_s, t_r, last_s, last_r,
):
    space, tm = lax.axis_index("space"), lax.axis_index("tm")
    z, y, core = space // 4, lax.rem(space // 2, 2), lax.rem(space, 2)
    quad = lax.rem(space, 4)

    def in_z(d):
        return {"space": lax.rem(z + d, 8) * 4 + quad, "tm": tm}

    def in_quad(d):
        return {"space": z * 4 + (quad ^ d), "tm": tm}

    def in_chips(e, d):
        return {"space": (lax.rem(z + d, 8) * 4 + quad) ^ (2 * e), "tm": tm}

    def in_tm(e, d):
        return {"space": space ^ e, "tm": lax.rem(tm + d, 8)}

    def load(tile):
        lanes = pl.ds(tile * 128, 128)
        return (
            pltpu.make_async_copy(noise_h.at[:, :, lanes], noise_v.at[tile], noise_sem.at[tile]),
            pltpu.make_async_copy(vec_h.at[:, lanes, :], vec_v.at[tile], vec_sem.at[tile]),
        )

    barrier = pltpu.get_barrier_semaphore()
    for d in FAR_FIRST:
        pl.semaphore_signal(barrier, inc=1, device_id=in_z(d), device_id_type=MESH)
        pl.semaphore_signal(barrier, inc=1, device_id=in_tm(0, d), device_id_type=MESH)
    for d in range(1, 3):
        pl.semaphore_signal(barrier, inc=1, device_id=in_quad(d), device_id_type=MESH)

    small = (
        pltpu.make_async_copy(mom_h, mom_s, small_sem.at[0]),
        pltpu.make_async_copy(pair_h, pair_s, small_sem.at[1]),
    )
    for copy in small:
        copy.start()
    for tile in range(4):
        for copy in load(tile):
            copy.start()

    for k in range(5):
        hrow[k, 0] = jnp.zeros((64, 128), jnp.float32)
        hrow[k, 11] = jnp.zeros((64, 128), jnp.float32)
    for copy in small:
        copy.wait()
    for q in range(MOMS):
        for k in range(3):
            spread[k, q : q + 1, :] = jnp.full((1, 128), mom_s[k, q], jnp.int32)

    scale = 1.0 / math.sqrt(12 * 512 * 32)
    row = space * 512 // EXTENT + iota((MOMS, 128), 1)
    q0 = jnp.abs(spread[0])
    angle = (spread[1] * lax.rem(row, EXTENT) + spread[2] * (row // EXTENT)).astype(jnp.float32)
    angle = angle * jnp.float32(2.0 * math.pi / EXTENT)
    size = jnp.where(q0 == 0, scale, jnp.where(q0 == 1, scale / SIZE1, scale / SIZE2))
    phase_r, phase_i = jnp.cos(angle) * size, -jnp.sin(angle) * size
    left = iota((MOMS, 128), 1) < 64
    for r in range(12):
        kap_r[r] = jnp.broadcast_to(phase_r[:, r : r + 1], (MOMS, 128))
        column = jnp.broadcast_to(phase_i[:, r : r + 1], (MOMS, 128))
        kap_i[r] = jnp.where(left, column, -column)

    phase0 = lax.rem(space * 32, EXTENT)
    lane = lax.rem(iota((8, 128), 1), 64)
    kind = iota((8, 128), 0)
    harmonic = jnp.where(kind < 2, 1, 2)
    amplitude = jnp.where(kind < 2, SIZE1, SIZE2)
    flip = jnp.where(iota((64, 128), 1) < 64, -1.0, 1.0).astype(jnp.bfloat16)

    def tile_step(tile, _):
        for copy in load(tile):
            copy.wait()
        starts = [phase0 + tile * 128 + 64 * h for h in range(2)]
        firsts = [lax.rem(start, EXTENT) for start in starts]
        waves = []
        for first in firsts:
            turn = ((first + lane) * harmonic).astype(jnp.float32) * jnp.float32(2.0 * math.pi / EXTENT)
            wave = amplitude * jnp.where(kind % 2 == 0, jnp.cos(turn), jnp.sin(turn))
            waves.append(wave.astype(jnp.bfloat16))
        totals = [None, None]
        for a4 in range(3):
            n = [noise_v[tile, 4 * a4 + a].astype(jnp.float32).astype(jnp.bfloat16) for a in range(4)]
            for h in range(2):
                cut = slice(64 * h, 64 * h + 64)
                joined = [jnp.concatenate([n[k][:, cut], n[k + 1][:, cut]], axis=1) for k in (0, 2)]
                n4 = jnp.concatenate(joined, axis=1)
                z4_r, z4_i = jnp.abs(n4 - 2) - 1, jnp.abs(n4 - 1) - 1
                wave = [jnp.concatenate([waves[h][k : k + 1, :]] * 2, axis=1) for k in range(4)]
                left_r = [z4_r, z4_r * wave[0], z4_i * -wave[1], z4_r * wave[2], z4_i * -wave[3]]
                left_i = [z4_i, z4_i * wave[0], z4_r * wave[1], z4_i * wave[2], z4_r * wave[3]]
                right_r, right_i = [], []
                for a in range(4):
                    v = vec_v[tile, 4 * a4 + a, 64 * h : 64 * h + 64, :]
                    t = swap_halves(v) * flip
                    for part, into in ((v, right_r), (t, right_i)):
                        for g in range(4):
                            piece = part[16 * g : 16 * g + 16]
                            zero = jnp.zeros_like(piece)
                            if g == 0:
                                pair = [piece, zero]
                            elif g == 3:
                                pair = [zero, piece]
                            else:
                                in_first = firsts[h] + 16 * g < EXTENT
                                pair = [jnp.where(in_first, piece, zero), jnp.where(in_first, zero, piece)]
                            into.append(jnp.concatenate(pair, axis=1))
                for lhs, rhs in ((left_r, right_r), (left_i, right_i)):
                    product = jnp.dot(
                        jnp.concatenate(lhs, axis=0), jnp.concatenate(rhs, axis=0), preferred_element_type=jnp.float32
                    )
                    totals[h] = product if totals[h] is None else totals[h] + product
        for h in range(2):
            f = [totals[h][64 * k : 64 * k + 64, :] for k in range(5)]
            terms = [f[3] + f[4], f[1] + f[2], f[0], f[1] - f[2], f[3] - f[4]]
            fresh = firsts[h] == 0 if h == 1 else (firsts[h] == 0) | (tile == 0)
            for k in range(5):
                at = starts[h] // EXTENT
                hrow[k, at] = jnp.where(fresh, 0.0, hrow[k, at]) + terms[k][:, 0:128]
                hrow[k, at + 1] = terms[k][:, 128:256]
        return 0

    lax.fori_loop(0, 4, tile_step, 0)
    pl.semaphore_wait(barrier, 16)

    def to_core(g):
        return pltpu.make_async_remote_copy(
            src_ref=raw.at[1 - core, g], dst_ref=core_in.at[g], send_sem=core_s.at[0], recv_sem=core_r.at[g],
            device_id=in_quad(1), device_id_type=MESH,
        )

    def to_y(g):
        return pltpu.make_async_remote_copy(
            src_ref=half.at[g, 1 - y], dst_ref=y_in.at[g], send_sem=y_s.at[0], recv_sem=y_r.at[g],
            device_id=in_quad(2), device_id_type=MESH,
        )

    def to_z(g, d):
        return pltpu.make_async_remote_copy(
            src_ref=own.at[g, lax.rem(z + d, 8)], dst_ref=z_in.at[g, d - 1],
            send_sem=z_s.at[0], recv_sem=z_r.at[g], device_id=in_z(d), device_id_type=MESH,
        )

    mine = core * 8 + tm

    def to_tm(g, e, d):
        return pltpu.make_async_remote_copy(
            src_ref=slices.at[g, mine], dst_ref=slices.at[g, mine],
            send_sem=t_s.at[0], recv_sem=t_r.at[g], device_id=in_tm(e, d), device_id_type=MESH,
        )

    def arrive(ref, sem):
        pltpu.make_async_copy(ref, ref, sem).wait()

    def momentum(g, k):
        q = lax.min(4 * g + k, MOMS - 1)
        q0 = mom_s[0, q] + 2
        acc_r = [jnp.zeros((8, 128), jnp.float32) for _ in range(8)]
        acc_i = [jnp.zeros((8, 128), jnp.float32) for _ in range(8)]
        for r in range(12):
            k_r = jnp.broadcast_to(kap_r[r, pl.ds(q, 1), :], (8, 128))
            k_i = jnp.broadcast_to(kap_i[r, pl.ds(q, 1), :], (8, 128))
            for i in range(8):
                part = hrow[q0, r, 8 * i : 8 * i + 8, :]
                acc_r[i] += k_r * part
                acc_i[i] += k_i * part
        tiles = [acc_r[i] + swap_halves(acc_i[i]) for i in range(8)]
        by_core = [swapped(tiles[2 * i], tiles[2 * i + 1], 2) for i in range(4)]
        for c in range(2):
            for i in range(2):
                by_y = swapped(by_core[2 * i][c], by_core[2 * i + 1][c], 4)
                for yy in range(2):
                    raw[c, g, yy, k, 8 * i : 8 * i + 8, :] = by_y[yy]

    def after_core(g):
        to_core(g).wait_recv()
        for yy in range(2):
            half[g, yy] = raw[core, g, yy] + core_in[g, yy]
        to_y(g).start()

    def first_step(g, _):
        for k in range(4):
            momentum(g, k)
        to_core(g).start()

        @pl.when(g >= LAG)
        def _():
            after_core(g - LAG)

        return 0

    lax.fori_loop(0, CHUNKS, first_step, 0)
    for g in range(CHUNKS - LAG, CHUNKS):
        after_core(g)

    def after_y(g, _):
        to_y(g).wait_recv()
        sums = half[g, y] + y_in[g]
        for top in range(2):
            tiles = [sums[k, 8 * top : 8 * top + 8, :] for k in range(4)]
            low = [swapped(tiles[2 * k], tiles[2 * k + 1], 2) for k in range(2)]
            for bit in range(2):
                pair = swapped(low[0][bit], low[1][bit], 4)
                for upper in range(2):
                    own[g, 4 * top + 2 * upper + bit] = pair[upper]
        for d in FAR_FIRST:
            to_z(g, d).start()
        return 0

    lax.fori_loop(0, CHUNKS, after_y, 0)

    def after_z(g, _):
        arrive(z_in.at[g], z_r.at[g])
        total = own[g, z]
        for d in range(7):
            total += z_in[g, d]
        for k in range(4):
            for c in range(2):
                mesons[c, 4 * g + k] = total[2 * k : 2 * k + 2, 64 * c : 64 * c + 64]
        slices[g, mine] = total
        for e, d in OTHERS:
            to_tm(g, e, d).start()
        return 0

    lax.fori_loop(0, CHUNKS, after_z, 0)

    lanes = iota((8, 128), 1)

    def after_tm(g, sums):
        arrive(slices.at[g, pl.ds(0, 15)], t_r.at[g])
        for c in range(2):
            for t in range(8):
                tile = slices[g, 8 * c + t]
                here[t, c] = tile
                turned[t, c] = swap_halves(jnp.where(lanes < 64, tile, -tile))
        for k in range(8):
            sink, source, rotated = here[pair_s[1, k]], here[pair_s[0, k]], turned[pair_s[0, k]]
            for c, term in enumerate((sink * source, sink * rotated)):
                value = jnp.sum(term[0] + term[1], axis=1, keepdims=True)
                sums = jnp.where(lanes == 16 * g + 2 * k + c, value, sums)
        return sums

    result = lax.fori_loop(0, CHUNKS, after_tm, jnp.zeros((8, 128), jnp.float32))
    result = result + pltpu.roll(result, 7, 0)
    chip = z * 2 + y

    def to_chip(e, d):
        return pltpu.make_async_remote_copy(
            src_ref=chips.at[chip], dst_ref=chips.at[chip], send_sem=last_s.at[0], recv_sem=last_r.at[0],
            device_id=in_chips(e, d), device_id_type=MESH,
        )

    for k in range(4):
        chips[chip, k : k + 1, :] = result[2 * k : 2 * k + 1, :]
    for e, d in OTHERS:
        to_chip(e, d).start()
    arrive(chips.at[pl.ds(0, 15)], last_r.at[0])
    total = chips[0]
    for k in range(1, 16):
        total += chips[k]
    columns = jnp.transpose(jnp.concatenate([total, total], axis=0) * (1.0 / 64))
    by_moment = jnp.concatenate([columns[16 * g : 16 * g + 16, 0:4] for g in range(CHUNKS)], axis=1)
    for k in range(8):
        traces[k] = by_moment[2 * k : 2 * k + 2, 0:MOMS]

    arrive(raw.at[0], core_s.at[0])
    arrive(y_in, y_s.at[0])
    arrive(z_in, z_s.at[0])
    arrive(slices.at[:, pl.ds(0, 15)], t_s.at[0])
    arrive(chips.at[pl.ds(0, 15)], last_s.at[0])


def write_kernel(mesons_v, traces_v, mesons_h, traces_h, sem):
    copies = (
        pltpu.make_async_copy(mesons_v.at[:, pl.ds(0, MOMS)], mesons_h, sem.at[0]),
        pltpu.make_async_copy(traces_v, traces_h, sem.at[1]),
    )
    for copy in copies:
        copy.start()
    for copy in copies:
        copy.wait()


def local(solutions, noise, momenta, pairs):
    f32, bf16 = jnp.float32, jnp.bfloat16
    vmem = pl.BlockSpec(memory_space=pltpu.VMEM)
    hbm = pl.BlockSpec(memory_space=pltpu.HBM)
    dma = pltpu.SemaphoreType.DMA
    mesons, traces = pl.pallas_call(
        fields_kernel,
        out_shape=(
            pltpu.VMEM((2, 4 * CHUNKS, 2, 64), f32),
            pltpu.VMEM((8, 2, MOMS), f32),
        ),
        in_specs=[hbm] * 4,
        out_specs=(vmem, vmem),
        scratch_shapes=[
            pltpu.SMEM((3, MOMS), jnp.int32),
            pltpu.SMEM((2, 8), jnp.int32),
            pltpu.VMEM((3, MOMS, 128), jnp.int32),
            pltpu.VMEM((4, 12, 64, 128), jnp.int32),
            pltpu.VMEM((4, 12, 128, 128), bf16),
            pltpu.VMEM((5, 12, 64, 128), f32),
            pltpu.VMEM((12, MOMS, 128), f32),
            pltpu.VMEM((12, MOMS, 128), f32),
            pltpu.VMEM((2, CHUNKS, 2, 4, 16, 128), f32),
            pltpu.VMEM((CHUNKS, 2, 4, 16, 128), f32),
            pltpu.VMEM((CHUNKS, 2, 4, 16, 128), f32),
            pltpu.VMEM((CHUNKS, 4, 16, 128), f32),
            pltpu.VMEM((CHUNKS, 8, 8, 128), f32),
            pltpu.VMEM((CHUNKS, 7, 8, 128), f32),
            pltpu.VMEM((CHUNKS, 16, 8, 128), f32),
            pltpu.VMEM((8, 2, 8, 128), f32),
            pltpu.VMEM((8, 2, 8, 128), f32),
            pltpu.VMEM((16, 4, 128), f32),
            dma((2,)), dma((4,)), dma((4,)),
            dma((1,)), dma((CHUNKS,)),
            dma((1,)), dma((CHUNKS,)),
            dma((1,)), dma((CHUNKS,)),
            dma((1,)), dma((CHUNKS,)),
            dma((1,)), dma((1,)),
        ],
        compiler_params=pltpu.CompilerParams(
            collective_id=0, has_side_effects=True, vmem_limit_bytes=66700000
        ),
        name="meson_fields",
    )(momenta.T, pairs.T, noise[0].transpose(1, 0, 2), solutions[0])
    mesons, correlators = pl.pallas_call(
        write_kernel,
        out_shape=(
            jax.ShapeDtypeStruct((2, MOMS, 2, 64), f32),
            jax.ShapeDtypeStruct((8, 2, MOMS), f32),
        ),
        in_specs=[vmem] * 2,
        out_specs=(hbm, hbm),
        scratch_shapes=[dma((2,))],
        compiler_params=pltpu.CompilerParams(vmem_limit_bytes=1 << 20),
        name="write_out",
    )(mesons, traces)
    return (mesons[None], correlators)


def solution(mesh):
    in_specs = (P("tm", None, "space", None), P("tm", None, None, "space"), P(), P("tm", None))
    out_specs = (P("tm", None, None, "space", None), P("tm", None, None))
    return jax.shard_map(local, mesh=mesh, in_specs=in_specs, out_specs=out_specs, check_vma=False)
```

```python
import math

import jax
import jax.numpy as jnp
from jax import lax
from jax.experimental import pallas as pl
from jax.experimental.pallas import tpu as pltpu
from jax.sharding import PartitionSpec as P

EXTENT = 48
MOMS = 27
CHUNKS = 7
LAG = 1
SIZE1, SIZE2 = 1.625, 1.1325
MESH = pl.DeviceIdType.MESH
FAR_FIRST = (4, 3, 5, 2, 6, 1, 7)
OTHERS = [(e, d) for d in FAR_FIRST for e in (1, 0)] + [(1, 0)]


def iota(shape, dim):
    return lax.broadcasted_iota(jnp.int32, shape, dim)


def swap_halves(array):
    return jnp.concatenate([array[:, 64:], array[:, :64]], axis=1)


def swapped(low, high, bit):
    has_bit = (iota((8, 128), 0) & bit) != 0
    return (
        jnp.where(has_bit, pltpu.roll(high, bit, 0), low),
        jnp.where(has_bit, high, pltpu.roll(low, 8 - bit, 0)),
    )


def fields_kernel(
    mom_h, pair_h, noise_h, vec_h, mesons, traces,
    mom_s, pair_s, spread, noise_v, vec_v, hrow, kap_r, kap_i,
    raw, core_in, half, y_in, own, z_in, slices, here, turned, chips,
    small_sem, noise_sem, vec_sem, core_s, core_r, y_s, y_r, z_s, z_r, t_s, t_r, last_s, last_r,
):
    space, tm = lax.axis_index("space"), lax.axis_index("tm")
    z, y, core = space // 4, lax.rem(space // 2, 2), lax.rem(space, 2)
    quad = lax.rem(space, 4)

    def in_z(d):
        return {"space": lax.rem(z + d, 8) * 4 + quad, "tm": tm}

    def in_quad(d):
        return {"space": z * 4 + (quad ^ d), "tm": tm}

    def in_chips(e, d):
        return {"space": (lax.rem(z + d, 8) * 4 + quad) ^ (2 * e), "tm": tm}

    def in_tm(e, d):
        return {"space": space ^ e, "tm": lax.rem(tm + d, 8)}

    def load(tile):
        lanes = pl.ds(tile * 128, 128)
        return (
            pltpu.make_async_copy(noise_h.at[:, :, lanes], noise_v.at[tile], noise_sem.at[tile]),
            pltpu.make_async_copy(vec_h.at[:, lanes, :], vec_v.at[tile], vec_sem.at[tile]),
        )

    small = (
        pltpu.make_async_copy(mom_h, mom_s, small_sem.at[0]),
        pltpu.make_async_copy(pair_h, pair_s, small_sem.at[1]),
    )
    for copy in small:
        copy.start()
    for tile in range(4):
        for copy in load(tile):
            copy.start()

    barrier = pltpu.get_barrier_semaphore()
    for d in FAR_FIRST:
        pl.semaphore_signal(barrier, inc=1, device_id=in_z(d), device_id_type=MESH)
        pl.semaphore_signal(barrier, inc=1, device_id=in_tm(0, d), device_id_type=MESH)
    for d in range(1, 3):
        pl.semaphore_signal(barrier, inc=1, device_id=in_quad(d), device_id_type=MESH)

    for k in range(5):
        hrow[k, 0] = jnp.zeros((64, 128), jnp.float32)
        hrow[k, 11] = jnp.zeros((64, 128), jnp.float32)
    for copy in small:
        copy.wait()
    for q in range(MOMS):
        for k in range(3):
            spread[k, q : q + 1, :] = jnp.full((1, 128), mom_s[k, q], jnp.int32)

    scale = 1.0 / math.sqrt(12 * 512 * 32)
    row = space * 512 // EXTENT + iota((MOMS, 128), 1)
    q0 = jnp.abs(spread[0])
    angle = (spread[1] * lax.rem(row, EXTENT) + spread[2] * (row // EXTENT)).astype(jnp.float32)
    angle = angle * jnp.float32(2.0 * math.pi / EXTENT)
    size = jnp.where(q0 == 0, scale, jnp.where(q0 == 1, scale / SIZE1, scale / SIZE2))
    phase_r, phase_i = jnp.cos(angle) * size, -jnp.sin(angle) * size
    left = iota((MOMS, 128), 1) < 64
    for r in range(12):
        kap_r[r] = jnp.broadcast_to(phase_r[:, r : r + 1], (MOMS, 128))
        column = jnp.broadcast_to(phase_i[:, r : r + 1], (MOMS, 128))
        kap_i[r] = jnp.where(left, column, -column)

    phase0 = lax.rem(space * 32, EXTENT)
    lane = lax.rem(iota((8, 128), 1), 64)
    kind = iota((8, 128), 0)
    harmonic = jnp.where(kind < 2, 1, 2)
    amplitude = jnp.where(kind < 2, SIZE1, SIZE2)
    flip = jnp.where(iota((64, 128), 1) < 64, -1.0, 1.0).astype(jnp.bfloat16)

    def tile_step(tile, _):
        for copy in load(tile):
            copy.wait()
        starts = [phase0 + tile * 128 + 64 * h for h in range(2)]
        firsts = [lax.rem(start, EXTENT) for start in starts]
        waves = []
        for first in firsts:
            turn = ((first + lane) * harmonic).astype(jnp.float32) * jnp.float32(2.0 * math.pi / EXTENT)
            wave = amplitude * jnp.where(kind % 2 == 0, jnp.cos(turn), jnp.sin(turn))
            waves.append(wave.astype(jnp.bfloat16))
        totals = [None, None]
        for a4 in range(3):
            n = [noise_v[tile, 4 * a4 + a].astype(jnp.float32).astype(jnp.bfloat16) for a in range(4)]
            for h in range(2):
                cut = slice(64 * h, 64 * h + 64)
                joined = [jnp.concatenate([n[k][:, cut], n[k + 1][:, cut]], axis=1) for k in (0, 2)]
                n4 = jnp.concatenate(joined, axis=1)
                z4_r, z4_i = jnp.abs(n4 - 2) - 1, jnp.abs(n4 - 1) - 1
                wave = [jnp.concatenate([waves[h][k : k + 1, :]] * 2, axis=1) for k in range(4)]
                left_r = [z4_r, z4_r * wave[0], z4_i * -wave[1], z4_r * wave[2], z4_i * -wave[3]]
                left_i = [z4_i, z4_i * wave[0], z4_r * wave[1], z4_i * wave[2], z4_r * wave[3]]
                right_r, right_i = [], []
                for a in range(4):
                    v = vec_v[tile, 4 * a4 + a, 64 * h : 64 * h + 64, :]
                    t = swap_halves(v) * flip
                    for part, into in ((v, right_r), (t, right_i)):
                        for g in range(4):
                            piece = part[16 * g : 16 * g + 16]
                            zero = jnp.zeros_like(piece)
                            if g == 0:
                                pair = [piece, zero]
                            elif g == 3:
                                pair = [zero, piece]
                            else:
                                in_first = firsts[h] + 16 * g < EXTENT
                                pair = [jnp.where(in_first, piece, zero), jnp.where(in_first, zero, piece)]
                            into.append(jnp.concatenate(pair, axis=1))
                for lhs, rhs in ((left_r, right_r), (left_i, right_i)):
                    product = jnp.dot(
                        jnp.concatenate(lhs, axis=0), jnp.concatenate(rhs, axis=0), preferred_element_type=jnp.float32
                    )
                    totals[h] = product if totals[h] is None else totals[h] + product
        for h in range(2):
            f = [totals[h][64 * k : 64 * k + 64, :] for k in range(5)]
            terms = [f[3] + f[4], f[1] + f[2], f[0], f[1] - f[2], f[3] - f[4]]
            fresh = firsts[h] == 0 if h == 1 else (firsts[h] == 0) | (tile == 0)
            for k in range(5):
                at = starts[h] // EXTENT
                hrow[k, at] = jnp.where(fresh, 0.0, hrow[k, at]) + terms[k][:, 0:128]
                hrow[k, at + 1] = terms[k][:, 128:256]
        return 0

    lax.fori_loop(0, 4, tile_step, 0)

    def to_core(g):
        return pltpu.make_async_remote_copy(
            src_ref=raw.at[1 - core, g], dst_ref=core_in.at[g], send_sem=core_s.at[0], recv_sem=core_r.at[g],
            device_id=in_quad(1), device_id_type=MESH,
        )

    def to_y(g):
        return pltpu.make_async_remote_copy(
            src_ref=half.at[g, 1 - y], dst_ref=y_in.at[g], send_sem=y_s.at[0], recv_sem=y_r.at[g],
            device_id=in_quad(2), device_id_type=MESH,
        )

    def to_z(g, d):
        return pltpu.make_async_remote_copy(
            src_ref=own.at[g, lax.rem(z + d, 8)], dst_ref=z_in.at[g, d - 1],
            send_sem=z_s.at[0], recv_sem=z_r.at[g], device_id=in_z(d), device_id_type=MESH,
        )

    mine = core * 8 + tm

    def to_tm(g, e, d):
        return pltpu.make_async_remote_copy(
            src_ref=slices.at[g, mine], dst_ref=slices.at[g, mine],
            send_sem=t_s.at[0], recv_sem=t_r.at[g], device_id=in_tm(e, d), device_id_type=MESH,
        )

    def arrive(ref, sem):
        pltpu.make_async_copy(ref, ref, sem).wait()

    def momentum(g, k):
        q = lax.min(4 * g + k, MOMS - 1)
        q0 = mom_s[0, q] + 2
        acc_r = [jnp.zeros((8, 128), jnp.float32) for _ in range(8)]
        acc_i = [jnp.zeros((8, 128), jnp.float32) for _ in range(8)]
        for r in range(12):
            k_r = jnp.broadcast_to(kap_r[r, pl.ds(q, 1), :], (8, 128))
            k_i = jnp.broadcast_to(kap_i[r, pl.ds(q, 1), :], (8, 128))
            for i in range(8):
                part = hrow[q0, r, 8 * i : 8 * i + 8, :]
                acc_r[i] += k_r * part
                acc_i[i] += k_i * part
        tiles = [acc_r[i] + swap_halves(acc_i[i]) for i in range(8)]
        by_core = [swapped(tiles[2 * i], tiles[2 * i + 1], 2) for i in range(4)]
        for c in range(2):
            for i in range(2):
                by_y = swapped(by_core[2 * i][c], by_core[2 * i + 1][c], 4)
                for yy in range(2):
                    raw[c, g, yy, k, 8 * i : 8 * i + 8, :] = by_y[yy]

    def after_core(g):
        to_core(g).wait_recv()
        for yy in range(2):
            half[g, yy] = raw[core, g, yy] + core_in[g, yy]
        to_y(g).start()

    def first_step(g, _):
        for k in range(4):
            momentum(g, k)
        @pl.when(g == 0)
        def _():
            pl.semaphore_wait(barrier, 16)

        to_core(g).start()

        @pl.when(g >= LAG)
        def _():
            after_core(g - LAG)

        return 0

    lax.fori_loop(0, CHUNKS, first_step, 0)
    for g in range(CHUNKS - LAG, CHUNKS):
        after_core(g)

    def after_y(g, _):
        to_y(g).wait_recv()
        sums = half[g, y] + y_in[g]
        for top in range(2):
            tiles = [sums[k, 8 * top : 8 * top + 8, :] for k in range(4)]
            low = [swapped(tiles[2 * k], tiles[2 * k + 1], 2) for k in range(2)]
            for bit in range(2):
                pair = swapped(low[0][bit], low[1][bit], 4)
                for upper in range(2):
                    own[g, 4 * top + 2 * upper + bit] = pair[upper]
        for d in FAR_FIRST:
            to_z(g, d).start()
        return 0

    lax.fori_loop(0, CHUNKS, after_y, 0)

    def after_z(g, _):
        arrive(z_in.at[g], z_r.at[g])
        total = own[g, z]
        for d in range(7):
            total += z_in[g, d]
        for k in range(4):
            for c in range(2):
                mesons[c, 4 * g + k] = total[2 * k : 2 * k + 2, 64 * c : 64 * c + 64]
        slices[g, mine] = total
        for e, d in OTHERS:
            to_tm(g, e, d).start()
        return 0

    lax.fori_loop(0, CHUNKS, after_z, 0)

    lanes = iota((8, 128), 1)

    def after_tm(g, sums):
        arrive(slices.at[g, pl.ds(0, 15)], t_r.at[g])
        for c in range(2):
            for t in range(8):
                tile = slices[g, 8 * c + t]
                here[t, c] = tile
                turned[t, c] = swap_halves(jnp.where(lanes < 64, tile, -tile))
        for k in range(8):
            sink, source, rotated = here[pair_s[1, k]], here[pair_s[0, k]], turned[pair_s[0, k]]
            for c, term in enumerate((sink * source, sink * rotated)):
                value = jnp.sum(term[0] + term[1], axis=1, keepdims=True)
                sums = jnp.where(lanes == 16 * g + 2 * k + c, value, sums)
        return sums

    result = lax.fori_loop(0, CHUNKS, after_tm, jnp.zeros((8, 128), jnp.float32))
    result = result + pltpu.roll(result, 7, 0)
    chip = z * 2 + y

    def to_chip(e, d):
        return pltpu.make_async_remote_copy(
            src_ref=chips.at[chip], dst_ref=chips.at[chip], send_sem=last_s.at[0], recv_sem=last_r.at[0],
            device_id=in_chips(e, d), device_id_type=MESH,
        )

    for k in range(4):
        chips[chip, k : k + 1, :] = result[2 * k : 2 * k + 1, :]
    for e, d in OTHERS:
        to_chip(e, d).start()
    arrive(chips.at[pl.ds(0, 15)], last_r.at[0])
    total = chips[0]
    for k in range(1, 16):
        total += chips[k]
    columns = jnp.transpose(jnp.concatenate([total, total], axis=0) * (1.0 / 64))
    by_moment = jnp.concatenate([columns[16 * g : 16 * g + 16, 0:4] for g in range(CHUNKS)], axis=1)
    for k in range(8):
        traces[k] = by_moment[2 * k : 2 * k + 2, 0:MOMS]

    arrive(raw.at[0], core_s.at[0])
    arrive(y_in, y_s.at[0])
    arrive(z_in, z_s.at[0])
    arrive(slices.at[:, pl.ds(0, 15)], t_s.at[0])
    arrive(chips.at[pl.ds(0, 15)], last_s.at[0])


def write_kernel(mesons_v, traces_v, mesons_h, traces_h, sem):
    copies = (
        pltpu.make_async_copy(mesons_v.at[:, pl.ds(0, MOMS)], mesons_h, sem.at[0]),
        pltpu.make_async_copy(traces_v, traces_h, sem.at[1]),
    )
    for copy in copies:
        copy.start()
    for copy in copies:
        copy.wait()


def local(solutions, noise, momenta, pairs):
    f32, bf16 = jnp.float32, jnp.bfloat16
    vmem = pl.BlockSpec(memory_space=pltpu.VMEM)
    hbm = pl.BlockSpec(memory_space=pltpu.HBM)
    dma = pltpu.SemaphoreType.DMA
    mesons, traces = pl.pallas_call(
        fields_kernel,
        out_shape=(
            pltpu.VMEM((2, 4 * CHUNKS, 2, 64), f32),
            pltpu.VMEM((8, 2, MOMS), f32),
        ),
        in_specs=[hbm] * 4,
        out_specs=(vmem, vmem),
        scratch_shapes=[
            pltpu.SMEM((3, MOMS), jnp.int32),
            pltpu.SMEM((2, 8), jnp.int32),
            pltpu.VMEM((3, MOMS, 128), jnp.int32),
            pltpu.VMEM((4, 12, 64, 128), jnp.int32),
            pltpu.VMEM((4, 12, 128, 128), bf16),
            pltpu.VMEM((5, 12, 64, 128), f32),
            pltpu.VMEM((12, MOMS, 128), f32),
            pltpu.VMEM((12, MOMS, 128), f32),
            pltpu.VMEM((2, CHUNKS, 2, 4, 16, 128), f32),
            pltpu.VMEM((CHUNKS, 2, 4, 16, 128), f32),
            pltpu.VMEM((CHUNKS, 2, 4, 16, 128), f32),
            pltpu.VMEM((CHUNKS, 4, 16, 128), f32),
            pltpu.VMEM((CHUNKS, 8, 8, 128), f32),
            pltpu.VMEM((CHUNKS, 7, 8, 128), f32),
            pltpu.VMEM((CHUNKS, 16, 8, 128), f32),
            pltpu.VMEM((8, 2, 8, 128), f32),
            pltpu.VMEM((8, 2, 8, 128), f32),
            pltpu.VMEM((16, 4, 128), f32),
            dma((2,)), dma((4,)), dma((4,)),
            dma((1,)), dma((CHUNKS,)),
            dma((1,)), dma((CHUNKS,)),
            dma((1,)), dma((CHUNKS,)),
            dma((1,)), dma((CHUNKS,)),
            dma((1,)), dma((1,)),
        ],
        compiler_params=pltpu.CompilerParams(
            collective_id=0, has_side_effects=True, vmem_limit_bytes=66700000
        ),
        name="meson_fields",
    )(momenta.T, pairs.T, noise[0].transpose(1, 0, 2), solutions[0])
    mesons, correlators = pl.pallas_call(
        write_kernel,
        out_shape=(
            jax.ShapeDtypeStruct((2, MOMS, 2, 64), f32),
            jax.ShapeDtypeStruct((8, 2, MOMS), f32),
        ),
        in_specs=[vmem] * 2,
        out_specs=(hbm, hbm),
        scratch_shapes=[dma((2,))],
        compiler_params=pltpu.CompilerParams(vmem_limit_bytes=1 << 20),
        name="write_out",
    )(mesons, traces)
    return (mesons[None], correlators)


def solution(mesh):
    in_specs = (P("tm", None, "space", None), P("tm", None, None, "space"), P(), P("tm", None))
    out_specs = (P("tm", None, None, "space", None), P("tm", None, None))
    return jax.shard_map(local, mesh=mesh, in_specs=in_specs, out_specs=out_specs, check_vma=False)
```
